512 devices in a mesh: tm: 32 (over z, y_hi), lat: 16 (over x, y_lo, core).
Axes of the slice: x: 4, y: 4 (y_hi: 2, y_lo: 2; y = y_hi * 2 + y_lo), z: 16, core: 2. Of those that a mesh axis runs over, the one named last changes fastest.
Arguments:
- controls: float32 [32, 3, 512, 1024], P('tm', None, 'lat'), may hold values from -3 to 3
- background: float32 [3, 512, 1024], P(None, 'lat'), may hold values from -3 to 3
- observations: float32 [32, 4, 512, 1024], P('tm', None, 'lat'), may hold values from -3 to 3
- obs_count: int32 [32, 4, 512, 1024], P('tm', None, 'lat'), may hold values from 0 to 3
Outputs:
- slid_controls: float32 [32, 3, 512, 1024], P('tm', None, 'lat')
- gradient: float32 [32, 3, 512, 1024], P('tm', None, 'lat')
- cost: float32 [], replicated
The draws below stay inside these ranges and needn't reach their ends.
All inputs are finite; a program needn't handle non-finite values.
Results may differ from the reference program's by a relative error of at most 0.0001.
Values sent between devices are 32-bit elements; how exact they have to be, the bound alone decides.
A program may use at most 64 MiB of HBM per device.

```python
import jax
import jax.numpy as jnp
from jax import lax

LON = 1024
SUBSTEPS = 4
NLAT = 512
WINDOWS = 32


def plant(result, key, least, largest):
    spot = [jax.random.randint(jax.random.fold_in(key, axis), (), 0, length) for axis, length in enumerate(result.shape)]
    longest = result.shape.index(max(result.shape))
    beside = spot[:longest] + [(spot[longest] + 1) % result.shape[longest]] + spot[longest + 1:]
    return result.at[tuple(spot)].set(least).at[tuple(beside)].set(largest)


def block_scale(stream_key, extent, shards, smallest, top_value):
    factor_of = 1.0
    for axis_at, shards_of in shards:
        heights = jax.random.uniform(jax.random.fold_in(jax.random.fold_in(stream_key, 6), axis_at), (shards_of,), jnp.float32, smallest / len(shards), top_value / len(shards))
        factor_of = factor_of * jnp.repeat(jnp.exp(heights), extent[axis_at] // shards_of).reshape((-1,) + (1,) * (len(extent) - 1 - axis_at))
    return factor_of


def noise(own_key, dims, width, limit, cuts=(), held_as=jnp.bfloat16):
    gain = block_scale(own_key, dims, cuts, -0.22, 0.18) if cuts else 1.0
    array = jax.random.normal(own_key, dims, jnp.float32) * width * gain
    return jnp.minimum(jnp.maximum(array, -limit), limit).astype(held_as)


def setup_inputs(seed: int = 0) -> dict:
    key_of = jax.random.split(jax.random.key(seed), 5)
    return {
        "controls": noise(key_of[0], (WINDOWS, 3, NLAT, LON), 0.5, 3.0, ((0, 32), (2, 16)), jnp.float32),
        "background": noise(key_of[1], (3, NLAT, LON), 0.5, 3.0, ((1, 16),), jnp.float32),
        "observations": noise(key_of[2], (WINDOWS, SUBSTEPS, NLAT, LON), 0.5, 3.0, ((0, 32), (2, 16)), jnp.float32),
        "obs_count": plant(jax.random.randint(key_of[3], (WINDOWS, SUBSTEPS, NLAT, LON), 0, 4), jax.random.fold_in(key_of[3], 1), 0, 3).astype(jnp.int32),
    }


courant = 0.25
diffusion = 0.1
spin_scale = 0.3
obs_weight = 0.5
q_weight = 1.0
step_scale = 0.2
epsilon = 1e-06

def advance(extended, coriolis):
    center = extended[:, 1:-1]
    north = extended[:, 2:]
    south = extended[:, :-2]
    east = jnp.roll(center, -1, axis=2)
    west = jnp.roll(center, 1, axis=2)
    height, zonal, merid = (center[0], center[1], center[2])
    flux_east = east[1] * (1.0 + east[0])
    flux_west = west[1] * (1.0 + west[0])
    flux_north = north[2] * (1.0 + north[0])
    flux_south = south[2] * (1.0 + south[0])
    spread = north + south + east + west - 4.0 * center
    half = 0.5 * courant
    new_height = height - half * (flux_east - flux_west + flux_north - flux_south) + diffusion * spread[0]
    new_zonal = zonal - half * (east[0] - west[0]) + coriolis * merid - half * (zonal * (east[1] - west[1]) + merid * (north[1] - south[1])) + diffusion * spread[1]
    new_merid = merid - half * (north[0] - south[0]) - coriolis * zonal - half * (zonal * (east[2] - west[2]) + merid * (north[2] - south[2])) + diffusion * spread[2]
    return jnp.stack([new_height, new_zonal, new_merid])

def coriolis_rows(index, total):
    latitude = jnp.pi * ((index.astype(jnp.float32) + 0.5) / total - 0.5)
    return (spin_scale * jnp.sin(latitude))[:, None]

def integrate(state, counts, targets, coriolis):
    cost = jnp.zeros((), jnp.float32)
    for section in range(SUBSTEPS):
        state = advance(jnp.pad(state, ((0, 0), (1, 1), (0, 0))), coriolis)
        resid = state[0] - targets[section]
        cost = cost + 0.5 * jnp.sum(obs_weight * counts[section].astype(jnp.float32) * resid * resid)
    return (state, cost)

def reference(controls, background, observations, obs_count):
    coriolis = coriolis_rows(jnp.arange(NLAT, dtype=jnp.int32), NLAT)

    def forward(items):
        state, counts, targets = items
        return integrate(state, counts, targets, coriolis)
    finals, obs_costs = lax.map(forward, (controls, obs_count, observations))
    previous = jnp.concatenate([background[None], finals[:-1]], axis=0)
    misfit = controls - previous
    weighted = q_weight * misfit
    later = jnp.concatenate([weighted[1:], jnp.zeros_like(weighted[:1])], axis=0)

    def backward(items):
        state, counts, targets, incoming = items

        def total(start):
            return integrate(start, counts, targets, coriolis)
        outputs, pull = jax.vjp(total, state)
        return pull((-incoming, jnp.ones((), outputs[1].dtype)))[0]
    adjoint = lax.map(backward, (controls, obs_count, observations, later))
    gradient = weighted + adjoint
    cost = jnp.sum(obs_costs) + 0.5 * q_weight * jnp.sum(misfit * misfit)
    norm = jnp.sqrt(jnp.sum(gradient * gradient) / gradient.size + epsilon)
    updated = controls - step_scale * gradient / norm
    slid = jnp.concatenate([updated[1:], finals[-1:]], axis=0)
    return (slid, gradient, cost)
```

```python
import functools

import jax
import jax.numpy as jnp
from jax import lax
from jax.experimental import pallas as pl
from jax.experimental.pallas import tpu as pltpu
from jax.sharding import PartitionSpec as P

half = 0.125
diffusion = 0.1
spin_scale = 0.3
obs_weight = 0.5
step_scale = 0.2
epsilon = 1e-06

STEPS = 4
SUB, LANES = 8, 128
BLOCK = 8
MESH = pl.DeviceIdType.MESH


def east(x):
    near = pltpu.roll(x, LANES - 1, x.ndim - 1)
    far = pltpu.roll(near, SUB - 1, x.ndim - 2)
    lane = lax.broadcasted_iota(jnp.int32, x.shape, x.ndim - 1)
    return jnp.where(lane == LANES - 1, far, near)


def west(x):
    near = pltpu.roll(x, 1, x.ndim - 1)
    far = pltpu.roll(near, 1, x.ndim - 2)
    lane = lax.broadcasted_iota(jnp.int32, x.shape, x.ndim - 1)
    return jnp.where(lane == 0, far, near)


def kernel(
    windows,
    bands,
    rows,
    entries,
    x_hbm,
    bg_hbm,
    obs_hbm,
    cnt_hbm,
    slid_hbm,
    grad_hbm,
    cost_ref,
    xin,
    bg,
    obs,
    cnt,
    fol,
    S,
    L,
    WR,
    F,
    prev,
    adjn,
    edge,
    grad,
    slid,
    n1,
    n2,
    local,
    outs,
    send,
    recv,
    a_send,
    a_recv,
    n_sem,
    z_sem,
):
    tm, lat = lax.axis_index("tm"), lax.axis_index("lat")
    z, y_hi = tm // 2, tm % 2
    depth = windows // 2
    group = 2 * bands
    mine = y_hi * bands + lat
    total = rows * bands
    tiles = rows // SUB
    pad = STEPS + 1
    span = rows + 2 * STEPS
    plane = rows * SUB

    def at(t, l):
        return {"tm": t, "lat": l}

    def group_peer(d):
        g = lax.rem(mine + d, group)
        return at(2 * z + g // bands, g % bands)

    def z_peer(d):
        return at(2 * lax.rem(z + d + depth, depth) + y_hi, lat)

    has_prev, has_next = tm > 0, tm < windows - 1
    has_south, has_north = lat > 0, lat < bands - 1
    prev_dev, next_dev = at(tm - 1, lat), at(tm + 1, lat)
    south_dev, north_dev = at(tm, lat - 1), at(tm, lat + 1)

    loads = [
        pltpu.make_async_copy(x_hbm, xin, local.at[0]),
        pltpu.make_async_copy(obs_hbm, obs, local.at[1]),
        pltpu.make_async_copy(cnt_hbm, cnt, local.at[2]),
    ]
    load_bg = pltpu.make_async_copy(bg_hbm, bg, local.at[3])
    loads[0].start()
    barrier = pltpu.get_barrier_semaphore()

    def greet(d, carry):
        pl.semaphore_signal(barrier, inc=1, device_id=group_peer(d), device_id_type=MESH)
        return carry

    def greet_dev(dev):
        pl.semaphore_signal(barrier, inc=1, device_id=dev, device_id_type=MESH)

    greet_dev(at(2 * lax.rem(z + 2 * y_hi - 1 + depth, depth) + 1 - y_hi, lat))
    greet_dev(z_peer(1))
    greet_dev(z_peer(-1))
    lax.fori_loop(1, group, greet, 0)
    loads[1].start()
    loads[2].start()
    pl.when(tm == 0)(lambda: load_bg.start())

    row_tile = jnp.zeros((SUB, LANES), jnp.float32)

    def table(t, carry):
        index = lax.broadcasted_iota(jnp.int32, (SUB, LANES), 0) + (t * SUB + lat * rows - pad)
        f = spin_scale * jnp.sin(jnp.pi * ((index.astype(jnp.float32) + 0.5) / total - 0.5))
        for r in range(SUB):
            F[t * SUB + r] = jnp.broadcast_to(f[r : r + 1], (SUB, LANES))
        return carry

    lax.fori_loop(0, (span + 2 + SUB - 1) // SUB, table, 0)
    for c in range(3):
        for j in range(STEPS):
            S[j, c, 0] = row_tile
            S[j, c, span + 1] = row_tile
        for p in range(2):
            L[p, c, 0] = row_tile
            L[p, c, span + 1] = row_tile
        for b in range(1, pad):
            L[0, c, b] = row_tile
            L[0, c, b + rows + STEPS] = row_tile

    def zero_rows(ref, first):
        for c in range(3):
            for b in range(STEPS):
                ref[c, first + b] = row_tile

    def poles(ref):
        pl.when(lat == 0)(lambda: zero_rows(ref, 1))
        pl.when(lat == bands - 1)(lambda: zero_rows(ref, pad + rows))

    def tile_row(c, t, r):
        return pl.ds(c * plane + t * SUB * SUB + r, SUB, stride=SUB)

    def per_row(fn, carry=0):
        def body(t, carry):
            for r in range(SUB):
                carry = fn(t, r, carry)
            return carry

        return lax.fori_loop(0, tiles, body, carry)

    poles(S.at[0])
    loads[0].wait()

    def unpack(t, r, carry):
        for c in range(3):
            S[0, c, pad + t * SUB + r] = xin[tile_row(c, t, r), :]
        return carry

    per_row(unpack)
    pl.semaphore_wait(barrier, group - 1 + 3)

    def remote(src, dst, k, dev):
        return pltpu.make_async_remote_copy(
            src_ref=src,
            dst_ref=dst,
            send_sem=send.at[k],
            recv_sem=recv.at[k],
            device_id=dev,
            device_id_type=MESH,
        )

    top = pl.ds(pad + rows - STEPS, STEPS)
    low = pl.ds(pad, STEPS)
    above = pl.ds(pad + rows, STEPS)
    below = pl.ds(1, STEPS)
    halo_up = remote(S.at[0, :, top], S.at[0, :, below], 0, north_dev)
    halo_down = remote(S.at[0, :, low], S.at[0, :, above], 1, south_dev)
    control = remote(xin, fol, 2, prev_dev)
    center = pl.ds(pad, rows)
    final = [remote(S.at[STEPS, c, center], prev.at[c], 3 + c, next_dev) for c in range(3)]
    out = 0
    edge_up = remote(L.at[out, :, above], edge.at[0], 6, north_dev)
    edge_down = remote(L.at[out, :, below], edge.at[1], 7, south_dev)

    pl.when(has_north)(lambda: halo_up.start())
    pl.when(has_south)(lambda: halo_down.start())
    pl.when(has_prev)(lambda: control.start())

    def z_signal(k):
        for d in (2**k, -(2**k)):
            pl.semaphore_signal(
                z_sem.at[k], inc=1, device_id=z_peer(d), device_id_type=MESH
            )

    z_signal(0)
    pl.when(has_south)(lambda: halo_up.wait_recv())
    pl.when(has_north)(lambda: halo_down.wait_recv())

    def forward(j):
        def block(t, carry):
            b = 1 + t * BLOCK

            def rows_at(c, shift):
                return S[j, c, pl.ds(b + shift, BLOCK)]

            h, u, v = (rows_at(c, 0) for c in range(3))
            hn, un, vn = (rows_at(c, 1) for c in range(3))
            hs, us, vs = (rows_at(c, -1) for c in range(3))
            he, ue, ve = east(h), east(u), east(v)
            hw, uw, vw = west(h), west(u), west(v)
            f = F[pl.ds(b, BLOCK)]
            flux = ue * (1.0 + he) - uw * (1.0 + hw) + vn * (1.0 + hn) - vs * (1.0 + hs)
            S[j + 1, 0, pl.ds(b, BLOCK)] = (
                h - half * flux + diffusion * (hn + hs + he + hw - 4.0 * h)
            )
            S[j + 1, 1, pl.ds(b, BLOCK)] = (
                u
                - half * (he - hw + u * (ue - uw) + v * (un - us))
                + f * v
                + diffusion * (un + us + ue + uw - 4.0 * u)
            )
            S[j + 1, 2, pl.ds(b, BLOCK)] = (
                v
                - half * (hn - hs + u * (ve - vw) + v * (vn - vs))
                - f * u
                + diffusion * (vn + vs + ve + vw - 4.0 * v)
            )
            return carry

        lax.fori_loop(0, span // BLOCK, block, 0)
        poles(S.at[j + 1])

    for j in range(STEPS):
        forward(j)

    @pl.when(has_next)
    def _():
        for c in range(3):
            final[c].start()

    pl.semaphore_wait(z_sem.at[0], 2)
    z_signal(1)

    loads[1].wait()
    loads[2].wait()
    zero = jnp.zeros((SUB, LANES), jnp.float32)

    def observe(j):
        def fn(t, r, cost):
            resid = S[j + 1, 0, pad + t * SUB + r] - obs[tile_row(j, t, r), :]
            weighted = obs_weight * cnt[tile_row(j, t, r), :].astype(jnp.float32) * resid
            WR[j, t * SUB + r] = weighted
            return cost + weighted * resid

        return fn

    cost = zero
    for j in range(STEPS):
        cost = per_row(observe(j), cost)

    pl.semaphore_wait(z_sem.at[1], 2)
    z_signal(2)

    @pl.when(has_next)
    def _():
        control.wait_recv()

        def start(t, r, carry):
            i = t * SUB + r
            for c in range(3):
                back = S[STEPS, c, pad + i] - fol[tile_row(c, t, r), :]
                if c == 0:
                    back = back + WR[STEPS - 1, i]
                L[0, c, pad + i] = back
            return carry

        per_row(start)

    @pl.when(jnp.logical_not(has_next))
    def _():
        def start(t, r, carry):
            i = t * SUB + r
            L[0, 0, pad + i] = WR[STEPS - 1, i]
            L[0, 1, pad + i] = row_tile
            L[0, 2, pad + i] = row_tile
            return carry

        per_row(start)

    def backward(j, p):
        def block(t, carry):
            b = 1 + t * BLOCK

            def grads(c, shift):
                return L[p, c, pl.ds(b + shift, BLOCK)]

            def state(c, shift):
                return S[j, c, pl.ds(b + shift, BLOCK)]

            H, U, V = (grads(c, 0) for c in range(3))
            HN, UN, VN = (grads(c, 1) for c in range(3))
            HS, US, VS = (grads(c, -1) for c in range(3))
            HE, UE, VE = east(H), east(U), east(V)
            HW, UW, VW = west(H), west(U), west(V)
            h, u, v = (state(c, 0) for c in range(3))
            un, vn = state(1, 1), state(2, 1)
            us, vs = state(1, -1), state(2, -1)
            ue, ve = east(u), east(v)
            uw, vw = west(u), west(v)
            f = F[pl.ds(b, BLOCK)]
            along, across = HE - HW, HN - HS
            thick = 1.0 + h
            L[1 - p, 0, pl.ds(b, BLOCK)] = (
                H
                + half * (along * u + across * v + (UE - UW) + (VN - VS))
                + diffusion * (HN + HS + HE + HW - 4.0 * H)
            )
            L[1 - p, 1, pl.ds(b, BLOCK)] = (
                U
                - f * V
                + half
                * (
                    along * thick
                    - U * (ue - uw)
                    - V * (ve - vw)
                    + (UE * ue - UW * uw)
                    + (UN * vn - US * vs)
                )
                + diffusion * (UN + US + UE + UW - 4.0 * U)
            )
            L[1 - p, 2, pl.ds(b, BLOCK)] = (
                V
                + f * U
                + half
                * (
                    across * thick
                    - U * (un - us)
                    - V * (vn - vs)
                    + (VE * ue - VW * uw)
                    + (VN * vn - VS * vs)
                )
                + diffusion * (VN + VS + VE + VW - 4.0 * V)
            )
            return carry

        lax.fori_loop(0, span // BLOCK, block, 0)
        if j > 0:

            def inject(t, r, carry):
                i = t * SUB + r
                L[1 - p, 0, pad + i] = L[1 - p, 0, pad + i] + WR[j - 1, i]
                return carry

            per_row(inject)
            poles(L.at[1 - p])

    p = 0
    for j in reversed(range(STEPS)):
        backward(j, p)
        p = 1 - p

    pl.when(has_north)(lambda: edge_up.start())
    pl.when(has_south)(lambda: edge_down.start())

    @pl.when(tm == 0)
    def _():
        load_bg.wait()

        def fn(t, r, carry):
            for c in range(3):
                prev[c, t * SUB + r] = bg[tile_row(c, t, r), :]
            return carry

        per_row(fn)

    @pl.when(has_south)
    def _():
        edge_up.wait_recv()
        for c in range(3):
            L[p, c, low] = L[p, c, low] + edge[0, c]

    @pl.when(has_north)
    def _():
        edge_down.wait_recv()
        for c in range(3):
            L[p, c, top] = L[p, c, top] + edge[1, c]

    @pl.when(has_prev)
    def _():
        for c in range(3):
            final[c].wait_recv()

    def gradient(t, r, carry):
        squares, cost = carry
        i = t * SUB + r
        for c in range(3):
            misfit = S[0, c, pad + i] - prev[c, i]
            g = misfit + L[p, c, pad + i]
            grad[tile_row(c, t, r), :] = g
            squares = squares + g * g
            cost = cost + misfit * misfit
        return squares, cost

    squares, cost = per_row(gradient, (zero, cost))

    def fold(x):
        x = jnp.sum(x, axis=0, keepdims=True)
        return x + pltpu.roll(x, LANES // 2, 1)

    lane = lax.broadcasted_iota(jnp.int32, (1, LANES), 1)
    n1[mine] = jnp.where(lane < LANES // 2, fold(squares), fold(cost))
    pl.semaphore_wait(z_sem.at[2], 2)

    def share(ref, slot, k, dev):
        return pltpu.make_async_remote_copy(
            src_ref=ref.at[slot],
            dst_ref=ref.at[slot],
            send_sem=n_sem.at[k, 0],
            recv_sem=n_sem.at[k, 1],
            device_id=dev,
            device_id_type=MESH,
        )

    def share1(d, carry):
        share(n1, mine, 0, group_peer(d)).start()
        return carry

    lax.fori_loop(1, group, share1, 0)

    pieces = []
    for q in range(2):
        for c in range(3):
            k = len(pieces)
            part = pl.ds(q * rows // 2, rows // 2)
            pieces.append(
                pltpu.make_async_remote_copy(
                    src_ref=L.at[p, c, pl.ds(pad + q * rows // 2, rows // 2)],
                    dst_ref=adjn.at[c, part],
                    send_sem=a_send.at[k],
                    recv_sem=a_recv.at[k],
                    device_id=prev_dev,
                    device_id_type=MESH,
                )
            )

    @pl.when(has_prev)
    def _():
        for piece in pieces[:3]:
            piece.start()

    store_grad = pltpu.make_async_copy(grad, grad_hbm, outs.at[0])
    store_grad.start()

    def settle(ref, count, k):
        many = pltpu.make_async_remote_copy(
            src_ref=ref.at[pl.ds(0, count)],
            dst_ref=ref.at[pl.ds(0, count)],
            send_sem=n_sem.at[k, 0],
            recv_sem=n_sem.at[k, 1],
            device_id=group_peer(1),
            device_id_type=MESH,
        )
        return many

    settle(n1, group - 1, 0).wait_recv()
    n2[z] = jnp.sum(n1[...], axis=0)

    def share2(d, carry):
        share(n2, z, 1, z_peer(d)).start()
        return carry

    lax.fori_loop(1, depth, share2, 0)

    @pl.when(has_prev)
    def _():
        for piece in pieces[3:]:
            piece.start()

    settle(n2, depth - 1, 1).wait_recv()
    sums = jnp.sum(n2[...], axis=0)
    square_total = jnp.sum(jnp.where(lane < LANES // 2, sums, 0.0), axis=1, keepdims=True)
    cost_total = jnp.sum(jnp.where(lane < LANES // 2, 0.0, sums), axis=1, keepdims=True)
    cost_ref[...] = jnp.broadcast_to(0.5 * cost_total, (SUB, LANES))
    scale = step_scale / jnp.sqrt(square_total / entries + epsilon)
    scale = jnp.broadcast_to(scale, (SUB, LANES))

    @pl.when(has_next)
    def _():
        for piece in pieces:
            piece.wait_recv()

        def fn(t, r, carry):
            i = t * SUB + r
            for c in range(3):
                control = fol[tile_row(c, t, r), :]
                g = (control - S[STEPS, c, pad + i]) + adjn[c, i]
                slid[tile_row(c, t, r), :] = control - scale * g
            return carry

        per_row(fn)

    @pl.when(jnp.logical_not(has_next))
    def _():
        def fn(t, r, carry):
            for c in range(3):
                slid[tile_row(c, t, r), :] = S[STEPS, c, pad + t * SUB + r]
            return carry

        per_row(fn)

    store_slid = pltpu.make_async_copy(slid, slid_hbm, outs.at[1])
    store_slid.start()
    pl.when(has_north)(lambda: halo_up.wait_send())
    pl.when(has_south)(lambda: halo_down.wait_send())
    pl.when(has_north)(lambda: edge_up.wait_send())
    pl.when(has_south)(lambda: edge_down.wait_send())

    @pl.when(has_next)
    def _():
        for c in range(3):
            final[c].wait_send()

    @pl.when(has_prev)
    def _():
        control.wait_send()
        for piece in pieces:
            piece.wait_send()

    settle(n1, group - 1, 0).wait_send()
    settle(n2, depth - 1, 1).wait_send()
    store_grad.wait()
    store_slid.wait()


def to_tiles(x):
    c, rows, lon = x.shape
    x = x.reshape(c, rows // SUB, SUB, lon // LANES, LANES)
    return x.transpose(0, 1, 3, 2, 4).reshape(c * rows * lon // LANES, LANES)


def from_tiles(x, rows, lon):
    x = x.reshape(-1, rows // SUB, lon // LANES, SUB, LANES)
    return x.transpose(0, 1, 3, 2, 4).reshape(-1, rows, lon)


def per_device(controls, background, observations, obs_count):
    rows, lon = controls.shape[2:]
    windows, bands = lax.axis_size("tm"), lax.axis_size("lat")
    entries = float(windows * bands * controls[0].size)
    n = 3 * rows * lon // LANES
    m = STEPS * rows * lon // LANES
    high = rows + 2 * STEPS + 2
    vmem = lambda *shape: pltpu.VMEM(shape, jnp.float32)
    dma = pltpu.SemaphoreType.DMA
    shape = jax.ShapeDtypeStruct((n, LANES), jnp.float32)
    slid, grad, cost = pl.pallas_call(
        functools.partial(kernel, windows, bands, rows, entries),
        out_shape=(shape, shape, jax.ShapeDtypeStruct((SUB, LANES), jnp.float32)),
        in_specs=[pl.BlockSpec(memory_space=pl.ANY)] * 4,
        out_specs=(
            pl.BlockSpec(memory_space=pl.ANY),
            pl.BlockSpec(memory_space=pl.ANY),
            pl.BlockSpec(memory_space=pltpu.VMEM),
        ),
        scratch_shapes=[
            vmem(n, LANES),
            vmem(n, LANES),
            vmem(m, LANES),
            pltpu.VMEM((m, LANES), jnp.int32),
            vmem(n, LANES),
            vmem(STEPS + 1, 3, high, SUB, LANES),
            vmem(2, 3, high, SUB, LANES),
            vmem(STEPS, rows, SUB, LANES),
            vmem((high + SUB - 1) // SUB * SUB, SUB, LANES),
            vmem(3, rows, SUB, LANES),
            vmem(3, rows, SUB, LANES),
            vmem(2, 3, STEPS, SUB, LANES),
            vmem(n, LANES),
            vmem(n, LANES),
            vmem(2 * bands, 1, LANES),
            vmem(windows // 2, 1, LANES),
            dma((4,)),
            dma((2,)),
            dma((8,)),
            dma((8,)),
            dma((6,)),
            dma((6,)),
            dma((2, 2)),
            pltpu.SemaphoreType.REGULAR((3,)),
        ],
        compiler_params=pltpu.CompilerParams(collective_id=0, has_side_effects=True),
    )(
        to_tiles(controls[0]),
        to_tiles(background),
        to_tiles(observations[0]),
        to_tiles(obs_count[0]),
    )
    return (
        from_tiles(slid, rows, lon)[None],
        from_tiles(grad, rows, lon)[None],
        cost[0, 0],
    )


def solution(mesh):
    spec = P("tm", None, "lat", None)
    return jax.shard_map(
        per_device,
        mesh=mesh,
        in_specs=(spec, P(None, "lat", None), spec, spec),
        out_specs=(spec, spec, P()),
        check_vma=False,
    )
```

```python
import functools

import jax
import jax.numpy as jnp
from jax import lax
from jax.experimental import pallas as pl
from jax.experimental.pallas import tpu as pltpu
from jax.sharding import PartitionSpec as P

half = 0.125
diffusion = 0.1
spin_scale = 0.3
obs_weight = 0.5
step_scale = 0.2
epsilon = 1e-06

STEPS = 4
SUB, LANES = 8, 128
BLOCK = 20
EARLY, MIDDLE = 0, 3
MESH = pl.DeviceIdType.MESH


def east(x):
    near = pltpu.roll(x, LANES - 1, x.ndim - 1)
    far = pltpu.roll(near, SUB - 1, x.ndim - 2)
    lane = lax.broadcasted_iota(jnp.int32, x.shape, x.ndim - 1)
    return jnp.where(lane == LANES - 1, far, near)


def west(x):
    near = pltpu.roll(x, 1, x.ndim - 1)
    far = pltpu.roll(near, 1, x.ndim - 2)
    lane = lax.broadcasted_iota(jnp.int32, x.shape, x.ndim - 1)
    return jnp.where(lane == 0, far, near)


def kernel(
    windows,
    bands,
    rows,
    entries,
    x_hbm,
    bg_hbm,
    obs_hbm,
    cnt_hbm,
    slid,
    grad,
    cost_ref,
    xin,
    bg,
    obs,
    cnt,
    fol,
    S,
    L,
    WR,
    F,
    prev,
    adjn,
    edge,
    n1,
    n2,
    n3,
    local,
    send,
    recv,
    f_send,
    f_recv,
    a_send,
    a_recv,
    n_sem,
    z_sem,
):
    tm, lat = lax.axis_index("tm"), lax.axis_index("lat")
    z, y_hi = tm // 2, tm % 2
    depth = windows // 2
    x, y_lo, core = lat // 4, lat // 2 % 2, lat % 2
    y = 2 * y_hi + y_lo
    total = rows * bands
    tiles = rows // SUB
    pad = STEPS + 1
    span = rows + 2 * STEPS
    plane = rows * SUB

    def at(t, l):
        return {"tm": t, "lat": l}

    across = bands // 2
    slot = 2 * x + core

    def x_peer(d):
        i = lax.rem(slot + d, across)
        return at(tm, 4 * (i // 2) + 2 * y_lo + i % 2)

    def y_peer(d):
        i = lax.rem(y + d, 4)
        return at(2 * z + i // 2, 4 * x + 2 * (i % 2) + core)

    def z_peer(d):
        return at(2 * lax.rem(z + d + depth, depth) + y_hi, lat)

    has_prev, has_next = tm > 0, tm < windows - 1
    has_south, has_north = lat > 0, lat < bands - 1
    prev_dev, next_dev = at(tm - 1, lat), at(tm + 1, lat)
    south_dev, north_dev = at(tm, lat - 1), at(tm, lat + 1)

    loads = [
        pltpu.make_async_copy(x_hbm, xin, local.at[0]),
        pltpu.make_async_copy(obs_hbm, obs, local.at[1]),
        pltpu.make_async_copy(cnt_hbm, cnt, local.at[2]),
    ]
    load_bg = pltpu.make_async_copy(bg_hbm, bg, local.at[3])
    loads[0].start()
    barrier = pltpu.get_barrier_semaphore()

    def greet(dev):
        pl.semaphore_signal(barrier, inc=1, device_id=dev, device_id_type=MESH)

    z_below, z_above = z > 0, z < depth - 1
    pl.when(z_below & (y_hi == 0))(lambda: greet(prev_dev))
    pl.when(z_above & (y_hi == 1))(lambda: greet(next_dev))
    pl.when(z_below)(lambda: greet(z_peer(-1)))
    pl.when(z_above)(lambda: greet(z_peer(1)))
    greet(at(tm, lax.rem(lat + 1, bands)))
    greet(at(tm, lax.rem(lat + bands - 1, bands)))
    for d in range(1, 4):
        greet(y_peer(d))
    for d in range(1, across):
        greet(x_peer(d))
    loads[1].start()
    loads[2].start()
    pl.when(tm == 0)(lambda: load_bg.start())

    row_tile = jnp.zeros((SUB, LANES), jnp.float32)

    def table(t, carry):
        index = lax.broadcasted_iota(jnp.int32, (SUB, LANES), 0) + (t * SUB + lat * rows - pad)
        f = spin_scale * jnp.sin(jnp.pi * ((index.astype(jnp.float32) + 0.5) / total - 0.5))
        for r in range(SUB):
            F[t * SUB + r] = jnp.broadcast_to(f[r : r + 1], (SUB, LANES))
        return carry

    lax.fori_loop(0, (span + 2 + SUB - 1) // SUB, table, 0)
    for c in range(3):
        for j in range(STEPS):
            S[j, c, 0] = row_tile
            S[j, c, span + 1] = row_tile
        for p in range(2):
            L[p, c, 0] = row_tile
            L[p, c, span + 1] = row_tile
        for b in range(1, pad):
            L[0, c, b] = row_tile
            L[0, c, b + rows + STEPS] = row_tile

    def zero_rows(ref, first):
        for c in range(3):
            for b in range(STEPS):
                ref[c, first + b] = row_tile

    def poles(ref):
        pl.when(lat == 0)(lambda: zero_rows(ref, 1))
        pl.when(lat == bands - 1)(lambda: zero_rows(ref, pad + rows))

    def tile_row(c, t, r):
        return pl.ds(c * plane + t * SUB * SUB + r, SUB, stride=SUB)

    def per_row(fn, carry=0):
        def body(t, carry):
            for r in range(SUB):
                carry = fn(t, r, carry)
            return carry

        return lax.fori_loop(0, tiles, body, carry)

    poles(S.at[0])
    loads[0].wait()

    def unpack(t, r, carry):
        for c in range(3):
            S[0, c, pad + t * SUB + r] = xin[tile_row(c, t, r), :]
        return carry

    per_row(unpack)
    before = (z + depth - 1) // depth
    after = (2 * depth - 2 - z) // depth
    facing = (1 - y_hi) * before + y_hi * after
    pl.semaphore_wait(barrier, 2 + 3 + across - 1 + before + after + facing)

    def remote(src, dst, k, dev):
        return pltpu.make_async_remote_copy(
            src_ref=src,
            dst_ref=dst,
            send_sem=send.at[k],
            recv_sem=recv.at[k],
            device_id=dev,
            device_id_type=MESH,
        )

    top = pl.ds(pad + rows - STEPS, STEPS)
    low = pl.ds(pad, STEPS)
    above = pl.ds(pad + rows, STEPS)
    below = pl.ds(1, STEPS)
    halo_up = remote(S.at[0, :, top], S.at[0, :, below], 0, north_dev)
    halo_down = remote(S.at[0, :, low], S.at[0, :, above], 1, south_dev)
    control = remote(xin, fol, 2, prev_dev)
    final = []
    for q in range(2):
        for c in range(3):
            k = len(final)
            final.append(
                pltpu.make_async_remote_copy(
                    src_ref=S.at[STEPS, c, pl.ds(pad + q * rows // 2, rows // 2)],
                    dst_ref=prev.at[c, pl.ds(q * rows // 2, rows // 2)],
                    send_sem=f_send.at[k],
                    recv_sem=f_recv.at[k],
                    device_id=next_dev,
                    device_id_type=MESH,
                )
            )
    out = 0
    edge_up = remote(L.at[out, :, above], edge.at[0], 3, north_dev)
    edge_down = remote(L.at[out, :, below], edge.at[1], 4, south_dev)

    pl.when(has_north)(lambda: halo_up.start())
    pl.when(has_south)(lambda: halo_down.start())
    pl.when(has_prev)(lambda: control.start())

    def z_signal(k):
        d = 2**k
        for exists, e in ((z >= d, -d), (z < depth - d, d)):

            @pl.when(exists)
            def _():
                pl.semaphore_signal(
                    z_sem.at[k], inc=1, device_id=z_peer(e), device_id_type=MESH
                )

    def z_wait(k):
        d = 2**k
        pl.semaphore_wait(z_sem.at[k], (z + depth - d) // depth + (2 * depth - 1 - d - z) // depth)

    z_signal(0)
    pl.when(has_south)(lambda: halo_up.wait_recv())
    pl.when(has_north)(lambda: halo_down.wait_recv())

    def forward(j):
        def block(t, carry):
            b = 1 + t * BLOCK

            def rows_at(c, shift):
                return S[j, c, pl.ds(b + shift, BLOCK)]

            h, u, v = (rows_at(c, 0) for c in range(3))
            hn, un, vn = (rows_at(c, 1) for c in range(3))
            hs, us, vs = (rows_at(c, -1) for c in range(3))
            he, ue, ve = east(h), east(u), east(v)
            hw, uw, vw = west(h), west(u), west(v)
            f = F[pl.ds(b, BLOCK)]
            flux = ue * (1.0 + he) - uw * (1.0 + hw) + vn * (1.0 + hn) - vs * (1.0 + hs)
            S[j + 1, 0, pl.ds(b, BLOCK)] = (
                h - half * flux + diffusion * (hn + hs + he + hw - 4.0 * h)
            )
            S[j + 1, 1, pl.ds(b, BLOCK)] = (
                u
                - half * (he - hw + u * (ue - uw) + v * (un - us))
                + f * v
                + diffusion * (un + us + ue + uw - 4.0 * u)
            )
            S[j + 1, 2, pl.ds(b, BLOCK)] = (
                v
                - half * (hn - hs + u * (ve - vw) + v * (vn - vs))
                - f * u
                + diffusion * (vn + vs + ve + vw - 4.0 * v)
            )
            return carry

        lax.fori_loop(0, span // BLOCK, block, 0)
        poles(S.at[j + 1])

    for j in range(STEPS):
        forward(j)

    @pl.when(has_next)
    def _():
        for piece in final[:EARLY]:
            piece.start()

    z_wait(0)
    z_signal(1)

    loads[1].wait()
    loads[2].wait()
    zero = jnp.zeros((SUB, LANES), jnp.float32)

    def observe(j):
        def fn(t, r, cost):
            resid = S[j + 1, 0, pad + t * SUB + r] - obs[tile_row(j, t, r), :]
            weighted = obs_weight * cnt[tile_row(j, t, r), :].astype(jnp.float32) * resid
            WR[j, t * SUB + r] = weighted
            return cost + weighted * resid

        return fn

    cost = zero
    for j in range(STEPS):
        cost = per_row(observe(j), cost)

    @pl.when(has_next)
    def _():
        control.wait_recv()
        for piece in final[EARLY:MIDDLE]:
            piece.start()

        def start(t, r, carry):
            i = t * SUB + r
            for c in range(3):
                back = S[STEPS, c, pad + i] - fol[tile_row(c, t, r), :]
                if c == 0:
                    back = back + WR[STEPS - 1, i]
                L[0, c, pad + i] = back
            return carry

        per_row(start)

    @pl.when(jnp.logical_not(has_next))
    def _():
        def start(t, r, carry):
            i = t * SUB + r
            L[0, 0, pad + i] = WR[STEPS - 1, i]
            L[0, 1, pad + i] = row_tile
            L[0, 2, pad + i] = row_tile
            return carry

        per_row(start)

    def backward(j, p):
        def block(t, carry):
            b = 1 + t * BLOCK

            def grads(c, shift):
                return L[p, c, pl.ds(b + shift, BLOCK)]

            def state(c, shift):
                return S[j, c, pl.ds(b + shift, BLOCK)]

            H, U, V = (grads(c, 0) for c in range(3))
            HN, UN, VN = (grads(c, 1) for c in range(3))
            HS, US, VS = (grads(c, -1) for c in range(3))
            HE, UE, VE = east(H), east(U), east(V)
            HW, UW, VW = west(H), west(U), west(V)
            h, u, v = (state(c, 0) for c in range(3))
            un, vn = state(1, 1), state(2, 1)
            us, vs = state(1, -1), state(2, -1)
            ue, ve = east(u), east(v)
            uw, vw = west(u), west(v)
            f = F[pl.ds(b, BLOCK)]
            along, across = HE - HW, HN - HS
            thick = 1.0 + h
            L[1 - p, 0, pl.ds(b, BLOCK)] = (
                H
                + half * (along * u + across * v + (UE - UW) + (VN - VS))
                + diffusion * (HN + HS + HE + HW - 4.0 * H)
            )
            L[1 - p, 1, pl.ds(b, BLOCK)] = (
                U
                - f * V
                + half
                * (
                    along * thick
                    - U * (ue - uw)
                    - V * (ve - vw)
                    + (UE * ue - UW * uw)
                    + (UN * vn - US * vs)
                )
                + diffusion * (UN + US + UE + UW - 4.0 * U)
            )
            L[1 - p, 2, pl.ds(b, BLOCK)] = (
                V
                + f * U
                + half
                * (
                    across * thick
                    - U * (un - us)
                    - V * (vn - vs)
                    + (VE * ue - VW * uw)
                    + (VN * vn - VS * vs)
                )
                + diffusion * (VN + VS + VE + VW - 4.0 * V)
            )
            return carry

        lax.fori_loop(0, span // BLOCK, block, 0)
        if j > 0:

            def inject(t, r, carry):
                i = t * SUB + r
                L[1 - p, 0, pad + i] = L[1 - p, 0, pad + i] + WR[j - 1, i]
                return carry

            per_row(inject)
            poles(L.at[1 - p])

    p = 0
    for j in reversed(range(STEPS)):
        backward(j, p)
        p = 1 - p

    pl.when(has_north)(lambda: edge_up.start())
    pl.when(has_south)(lambda: edge_down.start())

    @pl.when(has_next)
    def _():
        for piece in final[MIDDLE:]:
            piece.start()

    z_wait(1)
    z_signal(2)

    @pl.when(tm == 0)
    def _():
        load_bg.wait()

        def fn(t, r, carry):
            for c in range(3):
                prev[c, t * SUB + r] = bg[tile_row(c, t, r), :]
            return carry

        per_row(fn)

    @pl.when(has_south)
    def _():
        edge_up.wait_recv()
        for c in range(3):
            L[p, c, low] = L[p, c, low] + edge[0, c]

    @pl.when(has_north)
    def _():
        edge_down.wait_recv()
        for c in range(3):
            L[p, c, top] = L[p, c, top] + edge[1, c]

    @pl.when(has_prev)
    def _():
        for piece in final:
            piece.wait_recv()

    def gradient(t, r, carry):
        squares, cost = carry
        i = t * SUB + r
        for c in range(3):
            misfit = S[0, c, pad + i] - prev[c, i]
            g = misfit + L[p, c, pad + i]
            grad[tile_row(c, t, r), :] = g
            squares = squares + g * g
            cost = cost + misfit * misfit
        return squares, cost

    squares, cost = per_row(gradient, (zero, cost))

    def fold(x):
        x = jnp.sum(x, axis=0, keepdims=True)
        return x + pltpu.roll(x, LANES // 2, 1)

    lane = lax.broadcasted_iota(jnp.int32, (1, LANES), 1)
    z_wait(2)
    z_signal(3)
    n1[slot] = jnp.where(lane < LANES // 2, fold(squares), fold(cost))

    def share(ref, i, k, dev):
        return pltpu.make_async_remote_copy(
            src_ref=ref.at[i],
            dst_ref=ref.at[i],
            send_sem=n_sem.at[k, 0],
            recv_sem=n_sem.at[k, 1],
            device_id=dev,
            device_id_type=MESH,
        )

    for d in range(1, across):
        share(n1, slot, 0, x_peer(d)).start()

    pieces = []
    for q in range(2):
        for c in range(3):
            k = len(pieces)
            part = pl.ds(q * rows // 2, rows // 2)
            pieces.append(
                pltpu.make_async_remote_copy(
                    src_ref=L.at[p, c, pl.ds(pad + q * rows // 2, rows // 2)],
                    dst_ref=adjn.at[c, part],
                    send_sem=a_send.at[k],
                    recv_sem=a_recv.at[k],
                    device_id=prev_dev,
                    device_id_type=MESH,
                )
            )

    @pl.when(has_prev)
    def _():
        for piece in pieces[:1]:
            piece.start()

    def settle(ref, count, k):
        many = pltpu.make_async_remote_copy(
            src_ref=ref.at[pl.ds(0, count)],
            dst_ref=ref.at[pl.ds(0, count)],
            send_sem=n_sem.at[k, 0],
            recv_sem=n_sem.at[k, 1],
            device_id=z_peer(1),
            device_id_type=MESH,
        )
        return many

    settle(n1, across - 1, 0).wait_recv()
    n2[y] = jnp.sum(n1[...], axis=0)
    for d in range(1, 4):
        share(n2, y, 1, y_peer(d)).start()

    @pl.when(has_prev)
    def _():
        for piece in pieces[1:3]:
            piece.start()

    z_wait(3)
    settle(n2, 3, 1).wait_recv()
    n3[z] = jnp.sum(n2[...], axis=0)

    def share3(d, carry):
        share(n3, z, 2, z_peer(d)).start()
        return carry

    lax.fori_loop(1, depth, share3, 0)

    @pl.when(has_prev)
    def _():
        for piece in pieces[3:]:
            piece.start()

    settle(n3, depth - 1, 2).wait_recv()
    sums = jnp.sum(n3[...], axis=0)
    square_total = jnp.sum(jnp.where(lane < LANES // 2, sums, 0.0), axis=1, keepdims=True)
    cost_total = jnp.sum(jnp.where(lane < LANES // 2, 0.0, sums), axis=1, keepdims=True)
    cost_ref[...] = jnp.broadcast_to(0.5 * cost_total, (SUB, LANES))
    scale = step_scale / jnp.sqrt(square_total / entries + epsilon)
    scale = jnp.broadcast_to(scale, (SUB, LANES))

    @pl.when(has_next)
    def _():
        for piece in pieces:
            piece.wait_recv()

        def fn(t, r, carry):
            i = t * SUB + r
            for c in range(3):
                control = fol[tile_row(c, t, r), :]
                g = (control - S[STEPS, c, pad + i]) + adjn[c, i]
                slid[tile_row(c, t, r), :] = control - scale * g
            return carry

        per_row(fn)

    @pl.when(jnp.logical_not(has_next))
    def _():
        def fn(t, r, carry):
            for c in range(3):
                slid[tile_row(c, t, r), :] = S[STEPS, c, pad + t * SUB + r]
            return carry

        per_row(fn)

    pl.when(has_north)(lambda: halo_up.wait_send())
    pl.when(has_south)(lambda: halo_down.wait_send())
    pl.when(has_north)(lambda: edge_up.wait_send())
    pl.when(has_south)(lambda: edge_down.wait_send())

    @pl.when(has_next)
    def _():
        for piece in final:
            piece.wait_send()

    @pl.when(has_prev)
    def _():
        control.wait_send()
        for piece in pieces:
            piece.wait_send()

    settle(n1, across - 1, 0).wait_send()
    settle(n2, 3, 1).wait_send()
    settle(n3, depth - 1, 2).wait_send()


def finish(slid, grad, cost, slid_hbm, grad_hbm, cost_ref, sem):
    stores = [
        pltpu.make_async_copy(slid, slid_hbm, sem.at[0]),
        pltpu.make_async_copy(grad, grad_hbm, sem.at[1]),
    ]
    for store in stores:
        store.start()
    cost_ref[0, 0] = jnp.max(cost[...])
    for store in stores:
        store.wait()


def to_tiles(x):
    c, rows, lon = x.shape
    x = x.reshape(c, rows // SUB, SUB, lon // LANES, LANES)
    return x.transpose(0, 1, 3, 2, 4).reshape(c * rows * lon // LANES, LANES)


def from_tiles(x, rows, lon):
    x = x.reshape(-1, rows // SUB, lon // LANES, SUB, LANES)
    return x.transpose(0, 1, 3, 2, 4).reshape(-1, rows, lon)


def per_device(controls, background, observations, obs_count):
    rows, lon = controls.shape[2:]
    windows, bands = lax.axis_size("tm"), lax.axis_size("lat")
    entries = float(windows * bands * controls[0].size)
    n = 3 * rows * lon // LANES
    m = STEPS * rows * lon // LANES
    high = rows + 2 * STEPS + 2
    vmem = lambda *shape: pltpu.VMEM(shape, jnp.float32)
    dma = pltpu.SemaphoreType.DMA
    held = pltpu.VMEM((n, LANES), jnp.float32)
    stored = jax.ShapeDtypeStruct((n, LANES), jnp.float32)
    whole = pl.BlockSpec(memory_space=pltpu.VMEM)
    anywhere = pl.BlockSpec(memory_space=pl.ANY)
    results = pl.pallas_call(
        functools.partial(kernel, windows, bands, rows, entries),
        out_shape=(held, held, pltpu.VMEM((SUB, LANES), jnp.float32)),
        in_specs=[anywhere] * 4,
        out_specs=(whole, whole, whole),
        scratch_shapes=[
            vmem(n, LANES),
            vmem(n, LANES),
            vmem(m, LANES),
            pltpu.VMEM((m, LANES), jnp.int32),
            vmem(n, LANES),
            vmem(STEPS + 1, 3, high, SUB, LANES),
            vmem(2, 3, high, SUB, LANES),
            vmem(STEPS, rows, SUB, LANES),
            vmem((high + SUB - 1) // SUB * SUB, SUB, LANES),
            vmem(3, rows, SUB, LANES),
            vmem(3, rows, SUB, LANES),
            vmem(2, 3, STEPS, SUB, LANES),
            vmem(bands // 2, 1, LANES),
            vmem(4, 1, LANES),
            vmem(windows // 2, 1, LANES),
            dma((4,)),
            dma((5,)),
            dma((5,)),
            dma((6,)),
            dma((6,)),
            dma((6,)),
            dma((6,)),
            dma((3, 2)),
            pltpu.SemaphoreType.REGULAR((4,)),
        ],
        compiler_params=pltpu.CompilerParams(collective_id=0, has_side_effects=True),
    )(
        to_tiles(controls[0]),
        to_tiles(background),
        to_tiles(observations[0]),
        to_tiles(obs_count[0]),
    )
    slid, grad, cost = pl.pallas_call(
        finish,
        out_shape=(stored, stored, jax.ShapeDtypeStruct((1, 1), jnp.float32)),
        in_specs=[whole] * 3,
        out_specs=(anywhere, anywhere, pl.BlockSpec(memory_space=pltpu.SMEM)),
        scratch_shapes=[dma((2,))],
    )(*(pltpu.with_memory_space_constraint(r, pltpu.VMEM) for r in results))
    return (
        from_tiles(slid, rows, lon)[None],
        from_tiles(grad, rows, lon)[None],
        cost[0, 0],
    )


def solution(mesh):
    spec = P("tm", None, "lat", None)
    return jax.shard_map(
        per_device,
        mesh=mesh,
        in_specs=(spec, P(None, "lat", None), spec, spec),
        out_specs=(spec, spec, P()),
        check_vma=False,
    )
```

```python
import functools

import jax
import jax.numpy as jnp
from jax import lax
from jax.experimental import pallas as pl
from jax.experimental.pallas import tpu as pltpu
from jax.sharding import PartitionSpec as P

half = 0.125
diffusion = 0.1
spin_scale = 0.3
obs_weight = 0.5
step_scale = 0.2
epsilon = 1e-06

STEPS = 4
SUB, LANES = 8, 128
BLOCK = 20
EARLY = 3
PACE = 4
MESH = pl.DeviceIdType.MESH


def east(x):
    near = pltpu.roll(x, LANES - 1, x.ndim - 1)
    far = pltpu.roll(near, SUB - 1, x.ndim - 2)
    lane = lax.broadcasted_iota(jnp.int32, x.shape, x.ndim - 1)
    return jnp.where(lane == LANES - 1, far, near)


def west(x):
    near = pltpu.roll(x, 1, x.ndim - 1)
    far = pltpu.roll(near, 1, x.ndim - 2)
    lane = lax.broadcasted_iota(jnp.int32, x.shape, x.ndim - 1)
    return jnp.where(lane == 0, far, near)


def kernel(
    windows,
    bands,
    rows,
    entries,
    x_hbm,
    bg_hbm,
    obs_hbm,
    cnt_hbm,
    slid,
    grad,
    cost_ref,
    xin,
    bg,
    obs,
    cnt,
    fol,
    S,
    L,
    WR,
    F,
    prev,
    adjn,
    edge,
    n1,
    n2,
    local,
    send,
    recv,
    f_send,
    f_recv,
    a_send,
    a_recv,
    n_sem,
    z_sem,
    x_sem,
):
    tm, lat = lax.axis_index("tm"), lax.axis_index("lat")
    z, y_hi = tm // 2, tm % 2
    depth = windows // 2
    x, y_lo, core = lat // 4, lat // 2 % 2, lat % 2
    y = 2 * y_hi + y_lo
    total = rows * bands
    tiles = rows // SUB
    pad = STEPS + 1
    span = rows + 2 * STEPS
    plane = rows * SUB

    def at(t, l):
        return {"tm": t, "lat": l}

    across = bands // 2
    slot = 2 * x + core

    def x_peer(d):
        i = lax.rem(slot + d, across)
        return at(tm, 4 * (i // 2) + 2 * y_lo + i % 2)

    mine = y * across + slot
    members = 4 * across

    def plane_peer(d):
        i = lax.rem(mine + d, members)
        j, k = i // across, i % across
        return at(2 * z + j // 2, 4 * (k // 2) + 2 * (j % 2) + k % 2)

    def y_peer(d):
        i = lax.rem(y + d, 4)
        return at(2 * z + i // 2, 4 * x + 2 * (i % 2) + core)

    def z_peer(d):
        return at(2 * lax.rem(z + d + depth, depth) + y_hi, lat)

    has_prev, has_next = tm > 0, tm < windows - 1
    has_south, has_north = lat > 0, lat < bands - 1
    prev_dev, next_dev = at(tm - 1, lat), at(tm + 1, lat)
    south_dev, north_dev = at(tm, lat - 1), at(tm, lat + 1)

    loads = [
        pltpu.make_async_copy(x_hbm, xin, local.at[0]),
        pltpu.make_async_copy(obs_hbm, obs, local.at[1]),
        pltpu.make_async_copy(cnt_hbm, cnt, local.at[2]),
    ]
    load_bg = pltpu.make_async_copy(bg_hbm, bg, local.at[3])
    loads[0].start()
    barrier = pltpu.get_barrier_semaphore()

    def greet(dev):
        pl.semaphore_signal(barrier, inc=1, device_id=dev, device_id_type=MESH)

    z_below, z_above = z > 0, z < depth - 1
    pl.when(z_below & (y_hi == 0))(lambda: greet(prev_dev))
    pl.when(z_above & (y_hi == 1))(lambda: greet(next_dev))
    pl.when(z_below)(lambda: greet(z_peer(-1)))
    pl.when(z_above)(lambda: greet(z_peer(1)))
    greet(at(tm, lax.rem(lat + 1, bands)))
    greet(at(tm, lax.rem(lat + bands - 1, bands)))
    for d in range(1, 4):
        greet(y_peer(d))
    for d in range(1, across):
        greet(x_peer(d))
    loads[1].start()
    loads[2].start()
    pl.when(tm == 0)(lambda: load_bg.start())

    row_tile = jnp.zeros((SUB, LANES), jnp.float32)

    def table(t, carry):
        index = lax.broadcasted_iota(jnp.int32, (SUB, LANES), 0) + (t * SUB + lat * rows - pad)
        f = spin_scale * jnp.sin(jnp.pi * ((index.astype(jnp.float32) + 0.5) / total - 0.5))
        for r in range(SUB):
            F[t * SUB + r] = jnp.broadcast_to(f[r : r + 1], (SUB, LANES))
        return carry

    lax.fori_loop(0, (span + 2 + SUB - 1) // SUB, table, 0)
    for c in range(3):
        for j in range(STEPS):
            S[j, c, 0] = row_tile
            S[j, c, span + 1] = row_tile
        for p in range(2):
            L[p, c, 0] = row_tile
            L[p, c, span + 1] = row_tile
        for b in range(1, pad):
            L[0, c, b] = row_tile
            L[0, c, b + rows + STEPS] = row_tile

    def zero_rows(ref, first):
        for c in range(3):
            for b in range(STEPS):
                ref[c, first + b] = row_tile

    def poles(ref):
        pl.when(lat == 0)(lambda: zero_rows(ref, 1))
        pl.when(lat == bands - 1)(lambda: zero_rows(ref, pad + rows))

    def tile_row(c, t, r):
        return pl.ds(c * plane + t * SUB * SUB + r, SUB, stride=SUB)

    def per_row(fn, carry=0):
        def body(t, carry):
            for r in range(SUB):
                carry = fn(t, r, carry)
            return carry

        return lax.fori_loop(0, tiles, body, carry)

    poles(S.at[0])
    loads[0].wait()

    def unpack(t, r, carry):
        for c in range(3):
            S[0, c, pad + t * SUB + r] = xin[tile_row(c, t, r), :]
        return carry

    per_row(unpack)
    before = (z + depth - 1) // depth
    after = (2 * depth - 2 - z) // depth
    facing = (1 - y_hi) * before + y_hi * after
    pl.semaphore_wait(barrier, 2 + 3 + across - 1 + before + after + facing)

    def remote(src, dst, k, dev):
        return pltpu.make_async_remote_copy(
            src_ref=src,
            dst_ref=dst,
            send_sem=send.at[k],
            recv_sem=recv.at[k],
            device_id=dev,
            device_id_type=MESH,
        )

    top = pl.ds(pad + rows - STEPS, STEPS)
    low = pl.ds(pad, STEPS)
    above = pl.ds(pad + rows, STEPS)
    below = pl.ds(1, STEPS)
    halo_up = remote(S.at[0, :, top], S.at[0, :, below], 0, north_dev)
    halo_down = remote(S.at[0, :, low], S.at[0, :, above], 1, south_dev)
    control = remote(xin, fol, 2, prev_dev)
    final = []
    for q in range(2):
        for c in range(3):
            k = len(final)
            final.append(
                pltpu.make_async_remote_copy(
                    src_ref=S.at[STEPS, c, pl.ds(pad + q * rows // 2, rows // 2)],
                    dst_ref=prev.at[c, pl.ds(q * rows // 2, rows // 2)],
                    send_sem=f_send.at[k],
                    recv_sem=f_recv.at[k],
                    device_id=next_dev,
                    device_id_type=MESH,
                )
            )
    out = 0
    edge_up = remote(L.at[out, :, above], edge.at[0], 3, north_dev)
    edge_down = remote(L.at[out, :, below], edge.at[1], 4, south_dev)

    pl.when(has_north)(lambda: halo_up.start())
    pl.when(has_south)(lambda: halo_down.start())
    pl.when(has_prev)(lambda: control.start())

    def z_signal(k):
        d = 2**k
        for exists, e in ((z >= d, -d), (z < depth - d, d)):

            @pl.when(exists)
            def _():
                pl.semaphore_signal(
                    z_sem.at[k], inc=1, device_id=z_peer(e), device_id_type=MESH
                )

    def z_wait(k):
        d = 2**k
        pl.semaphore_wait(z_sem.at[k], (z + depth - d) // depth + (2 * depth - 1 - d - z) // depth)

    z_signal(0)
    for d in range(1, across):
        pl.semaphore_signal(x_sem, inc=1, device_id=x_peer(d), device_id_type=MESH)
    pl.when(has_south)(lambda: halo_up.wait_recv())
    pl.when(has_north)(lambda: halo_down.wait_recv())

    def forward(j):
        def block(t, carry):
            b = 1 + t * BLOCK

            def rows_at(c, shift):
                return S[j, c, pl.ds(b + shift, BLOCK)]

            h, u, v = (rows_at(c, 0) for c in range(3))
            hn, un, vn = (rows_at(c, 1) for c in range(3))
            hs, us, vs = (rows_at(c, -1) for c in range(3))
            he, ue, ve = east(h), east(u), east(v)
            hw, uw, vw = west(h), west(u), west(v)
            f = F[pl.ds(b, BLOCK)]
            flux = ue * (1.0 + he) - uw * (1.0 + hw) + vn * (1.0 + hn) - vs * (1.0 + hs)
            S[j + 1, 0, pl.ds(b, BLOCK)] = (
                h - half * flux + diffusion * (hn + hs + he + hw - 4.0 * h)
            )
            S[j + 1, 1, pl.ds(b, BLOCK)] = (
                u
                - half * (he - hw + u * (ue - uw) + v * (un - us))
                + f * v
                + diffusion * (un + us + ue + uw - 4.0 * u)
            )
            S[j + 1, 2, pl.ds(b, BLOCK)] = (
                v
                - half * (hn - hs + u * (ve - vw) + v * (vn - vs))
                - f * u
                + diffusion * (vn + vs + ve + vw - 4.0 * v)
            )
            return carry

        lax.fori_loop(0, span // BLOCK, block, 0)
        poles(S.at[j + 1])

    for j in range(STEPS):
        forward(j)

    z_wait(0)
    z_signal(1)

    loads[1].wait()
    loads[2].wait()
    zero = jnp.zeros((SUB, LANES), jnp.float32)

    def observe(j):
        def fn(t, r, cost):
            resid = S[j + 1, 0, pad + t * SUB + r] - obs[tile_row(j, t, r), :]
            weighted = obs_weight * cnt[tile_row(j, t, r), :].astype(jnp.float32) * resid
            WR[j, t * SUB + r] = weighted
            return cost + weighted * resid

        return fn

    cost = zero
    for j in range(STEPS):
        cost = per_row(observe(j), cost)

    pl.when(has_prev)(lambda: control.wait_send())

    @pl.when(has_next)
    def _():
        control.wait_recv()
        for piece in final[:EARLY]:
            piece.start()

        def start(t, r, carry):
            i = t * SUB + r
            for c in range(3):
                back = S[STEPS, c, pad + i] - fol[tile_row(c, t, r), :]
                if c == 0:
                    back = back + WR[STEPS - 1, i]
                L[0, c, pad + i] = back
            return carry

        per_row(start)

    @pl.when(jnp.logical_not(has_next))
    def _():
        def start(t, r, carry):
            i = t * SUB + r
            L[0, 0, pad + i] = WR[STEPS - 1, i]
            L[0, 1, pad + i] = row_tile
            L[0, 2, pad + i] = row_tile
            return carry

        per_row(start)

    def backward(j, p):
        def block(t, carry):
            b = 1 + t * BLOCK

            def grads(c, shift):
                return L[p, c, pl.ds(b + shift, BLOCK)]

            def state(c, shift):
                return S[j, c, pl.ds(b + shift, BLOCK)]

            H, U, V = (grads(c, 0) for c in range(3))
            HN, UN, VN = (grads(c, 1) for c in range(3))
            HS, US, VS = (grads(c, -1) for c in range(3))
            HE, UE, VE = east(H), east(U), east(V)
            HW, UW, VW = west(H), west(U), west(V)
            h, u, v = (state(c, 0) for c in range(3))
            un, vn = state(1, 1), state(2, 1)
            us, vs = state(1, -1), state(2, -1)
            ue, ve = east(u), east(v)
            uw, vw = west(u), west(v)
            f = F[pl.ds(b, BLOCK)]
            along, across = HE - HW, HN - HS
            thick = 1.0 + h
            L[1 - p, 0, pl.ds(b, BLOCK)] = (
                H
                + half * (along * u + across * v + (UE - UW) + (VN - VS))
                + diffusion * (HN + HS + HE + HW - 4.0 * H)
            )
            L[1 - p, 1, pl.ds(b, BLOCK)] = (
                U
                - f * V
                + half
                * (
                    along * thick
                    - U * (ue - uw)
                    - V * (ve - vw)
                    + (UE * ue - UW * uw)
                    + (UN * vn - US * vs)
                )
                + diffusion * (UN + US + UE + UW - 4.0 * U)
            )
            L[1 - p, 2, pl.ds(b, BLOCK)] = (
                V
                + f * U
                + half
                * (
                    across * thick
                    - U * (un - us)
                    - V * (vn - vs)
                    + (VE * ue - VW * uw)
                    + (VN * vn - VS * vs)
                )
                + diffusion * (VN + VS + VE + VW - 4.0 * V)
            )
            return carry

        lax.fori_loop(0, span // BLOCK, block, 0)
        if j > 0:

            def inject(t, r, carry):
                i = t * SUB + r
                L[1 - p, 0, pad + i] = L[1 - p, 0, pad + i] + WR[j - 1, i]
                return carry

            per_row(inject)
            poles(L.at[1 - p])

    p = 0
    for j in reversed(range(STEPS)):
        backward(j, p)
        p = 1 - p

    pl.when(has_north)(lambda: edge_up.start())
    pl.when(has_south)(lambda: edge_down.start())

    @pl.when(has_next)
    def _():
        for piece in final[EARLY:]:
            piece.start()

    z_wait(1)
    z_signal(2)

    @pl.when(tm == 0)
    def _():
        load_bg.wait()

        def fn(t, r, carry):
            for c in range(3):
                prev[c, t * SUB + r] = bg[tile_row(c, t, r), :]
            return carry

        per_row(fn)

    @pl.when(has_south)
    def _():
        edge_up.wait_recv()
        for c in range(3):
            L[p, c, low] = L[p, c, low] + edge[0, c]

    @pl.when(has_north)
    def _():
        edge_down.wait_recv()
        for c in range(3):
            L[p, c, top] = L[p, c, top] + edge[1, c]

    pieces = []
    for q in range(2):
        for c in range(3):
            k = len(pieces)
            part = pl.ds(q * rows // 2, rows // 2)
            pieces.append(
                pltpu.make_async_remote_copy(
                    src_ref=L.at[p, c, pl.ds(pad + q * rows // 2, rows // 2)],
                    dst_ref=adjn.at[c, part],
                    send_sem=a_send.at[k],
                    recv_sem=a_recv.at[k],
                    device_id=prev_dev,
                    device_id_type=MESH,
                )
            )

    def send_pieces(first, last):
        @pl.when(has_prev)
        def _():
            for piece in pieces[first:last]:
                piece.start()

    z_wait(2)
    z_signal(3)

    @pl.when(has_prev)
    def _():
        for piece in final:
            piece.wait_recv()

    def gradient(t, r, carry):
        squares, cost = carry
        i = t * SUB + r
        for c in range(3):
            misfit = S[0, c, pad + i] - prev[c, i]
            g = misfit + L[p, c, pad + i]
            grad[tile_row(c, t, r), :] = g
            squares = squares + g * g
            cost = cost + misfit * misfit
        return squares, cost

    squares, cost = per_row(gradient, (zero, cost))

    def fold(x):
        x = jnp.sum(x, axis=0, keepdims=True)
        return x + pltpu.roll(x, LANES // 2, 1)

    lane = lax.broadcasted_iota(jnp.int32, (1, LANES), 1)
    pl.semaphore_wait(x_sem, across - 1)
    n1[mine] = jnp.where(lane < LANES // 2, fold(squares), fold(cost))

    def share(ref, i, k, dev):
        return pltpu.make_async_remote_copy(
            src_ref=ref.at[i],
            dst_ref=ref.at[i],
            send_sem=n_sem.at[k, 0],
            recv_sem=n_sem.at[k, 1],
            device_id=dev,
            device_id_type=MESH,
        )

    def share1(d, carry):
        share(n1, mine, 0, plane_peer(d)).start()
        return carry

    lax.fori_loop(1, members, share1, 0)

    @pl.when(has_next)
    def _():
        for piece in final:
            piece.wait_send()

    send_pieces(0, PACE)

    def settle(ref, count, k):
        many = pltpu.make_async_remote_copy(
            src_ref=ref.at[pl.ds(0, count)],
            dst_ref=ref.at[pl.ds(0, count)],
            send_sem=n_sem.at[k, 0],
            recv_sem=n_sem.at[k, 1],
            device_id=z_peer(1),
            device_id_type=MESH,
        )
        return many

    settle(n1, members - 1, 0).wait_recv()
    n2[z] = jnp.sum(n1[...], axis=0)
    z_wait(3)

    def share2(d, carry):
        share(n2, z, 1, z_peer(d)).start()
        return carry

    lax.fori_loop(1, depth, share2, 0)
    send_pieces(PACE, 6)
    settle(n2, depth - 1, 1).wait_recv()
    sums = jnp.sum(n2[...], axis=0)
    square_total = jnp.sum(jnp.where(lane < LANES // 2, sums, 0.0), axis=1, keepdims=True)
    cost_total = jnp.sum(jnp.where(lane < LANES // 2, 0.0, sums), axis=1, keepdims=True)
    cost_ref[...] = jnp.broadcast_to(0.5 * cost_total, (SUB, LANES))
    scale = step_scale / jnp.sqrt(square_total / entries + epsilon)
    scale = jnp.broadcast_to(scale, (SUB, LANES))

    @pl.when(has_next)
    def _():
        for piece in pieces:
            piece.wait_recv()

        def fn(t, r, carry):
            i = t * SUB + r
            for c in range(3):
                control = fol[tile_row(c, t, r), :]
                g = (control - S[STEPS, c, pad + i]) + adjn[c, i]
                slid[tile_row(c, t, r), :] = control - scale * g
            return carry

        per_row(fn)

    @pl.when(jnp.logical_not(has_next))
    def _():
        def fn(t, r, carry):
            for c in range(3):
                slid[tile_row(c, t, r), :] = S[STEPS, c, pad + t * SUB + r]
            return carry

        per_row(fn)

    pl.when(has_north)(lambda: halo_up.wait_send())
    pl.when(has_south)(lambda: halo_down.wait_send())
    pl.when(has_north)(lambda: edge_up.wait_send())
    pl.when(has_south)(lambda: edge_down.wait_send())

    @pl.when(has_prev)
    def _():
        for piece in pieces:
            piece.wait_send()

    settle(n1, members - 1, 0).wait_send()
    settle(n2, depth - 1, 1).wait_send()


def finish(slid, grad, cost, slid_hbm, grad_hbm, cost_ref, sem):
    stores = [
        pltpu.make_async_copy(slid, slid_hbm, sem.at[0]),
        pltpu.make_async_copy(grad, grad_hbm, sem.at[1]),
    ]
    for store in stores:
        store.start()
    cost_ref[0, 0] = jnp.max(cost[...])
    for store in stores:
        store.wait()


def to_tiles(x):
    c, rows, lon = x.shape
    x = x.reshape(c, rows // SUB, SUB, lon // LANES, LANES)
    return x.transpose(0, 1, 3, 2, 4).reshape(c * rows * lon // LANES, LANES)


def from_tiles(x, rows, lon):
    x = x.reshape(-1, rows // SUB, lon // LANES, SUB, LANES)
    return x.transpose(0, 1, 3, 2, 4).reshape(-1, rows, lon)


def per_device(controls, background, observations, obs_count):
    rows, lon = controls.shape[2:]
    windows, bands = lax.axis_size("tm"), lax.axis_size("lat")
    entries = float(windows * bands * controls[0].size)
    n = 3 * rows * lon // LANES
    m = STEPS * rows * lon // LANES
    high = rows + 2 * STEPS + 2
    vmem = lambda *shape: pltpu.VMEM(shape, jnp.float32)
    dma = pltpu.SemaphoreType.DMA
    held = pltpu.VMEM((n, LANES), jnp.float32)
    stored = jax.ShapeDtypeStruct((n, LANES), jnp.float32)
    whole = pl.BlockSpec(memory_space=pltpu.VMEM)
    anywhere = pl.BlockSpec(memory_space=pl.ANY)
    results = pl.pallas_call(
        functools.partial(kernel, windows, bands, rows, entries),
        out_shape=(held, held, pltpu.VMEM((SUB, LANES), jnp.float32)),
        in_specs=[anywhere] * 4,
        out_specs=(whole, whole, whole),
        scratch_shapes=[
            vmem(n, LANES),
            vmem(n, LANES),
            vmem(m, LANES),
            pltpu.VMEM((m, LANES), jnp.int32),
            vmem(n, LANES),
            vmem(STEPS + 1, 3, high, SUB, LANES),
            vmem(2, 3, high, SUB, LANES),
            vmem(STEPS, rows, SUB, LANES),
            vmem((high + SUB - 1) // SUB * SUB, SUB, LANES),
            vmem(3, rows, SUB, LANES),
            vmem(3, rows, SUB, LANES),
            vmem(2, 3, STEPS, SUB, LANES),
            vmem(2 * bands, 1, LANES),
            vmem(windows // 2, 1, LANES),
            dma((4,)),
            dma((5,)),
            dma((5,)),
            dma((6,)),
            dma((6,)),
            dma((6,)),
            dma((6,)),
            dma((2, 2)),
            pltpu.SemaphoreType.REGULAR((4,)),
            pltpu.SemaphoreType.REGULAR,
        ],
        compiler_params=pltpu.CompilerParams(collective_id=0, has_side_effects=True),
    )(
        to_tiles(controls[0]),
        to_tiles(background),
        to_tiles(observations[0]),
        to_tiles(obs_count[0]),
    )
    slid, grad, cost = pl.pallas_call(
        finish,
        out_shape=(stored, stored, jax.ShapeDtypeStruct((1, 1), jnp.float32)),
        in_specs=[whole] * 3,
        out_specs=(anywhere, anywhere, pl.BlockSpec(memory_space=pltpu.SMEM)),
        scratch_shapes=[dma((2,))],
    )(*(pltpu.with_memory_space_constraint(r, pltpu.VMEM) for r in results))
    return (
        from_tiles(slid, rows, lon)[None],
        from_tiles(grad, rows, lon)[None],
        cost[0, 0],
    )


def solution(mesh):
    spec = P("tm", None, "lat", None)
    return jax.shard_map(
        per_device,
        mesh=mesh,
        in_specs=(spec, P(None, "lat", None), spec, spec),
        out_specs=(spec, spec, P()),
        check_vma=False,
    )
```

```python
import functools

import jax
import jax.numpy as jnp
from jax import lax
from jax.experimental import pallas as pl
from jax.experimental.pallas import tpu as pltpu
from jax.sharding import PartitionSpec as P

half = 0.125
diffusion = 0.1
spin_scale = 0.3
obs_weight = 0.5
step_scale = 0.2
epsilon = 1e-06

STEPS = 4
SUB, LANES = 8, 128
BLOCK = 20
CHUNKS = 3
EARLY = 3
PACE = 4
MESH = pl.DeviceIdType.MESH


def east(x):
    near = pltpu.roll(x, LANES - 1, x.ndim - 1)
    far = pltpu.roll(near, SUB - 1, x.ndim - 2)
    lane = lax.broadcasted_iota(jnp.int32, x.shape, x.ndim - 1)
    return jnp.where(lane == LANES - 1, far, near)


def west(x):
    near = pltpu.roll(x, 1, x.ndim - 1)
    far = pltpu.roll(near, 1, x.ndim - 2)
    lane = lax.broadcasted_iota(jnp.int32, x.shape, x.ndim - 1)
    return jnp.where(lane == 0, far, near)


def kernel(
    windows,
    bands,
    rows,
    entries,
    x_hbm,
    bg_hbm,
    obs_hbm,
    cnt_hbm,
    start_ref,
    slope,
    grad,
    scale_ref,
    cost_ref,
    xin,
    bg,
    obs,
    cnt,
    fol,
    S,
    L,
    WR,
    F,
    prev,
    adjn,
    edge,
    n1,
    n2,
    local,
    send,
    recv,
    f_send,
    f_recv,
    a_send,
    a_recv,
    n_sem,
    z_sem,
    x_sem,
):
    tm, lat = lax.axis_index("tm"), lax.axis_index("lat")
    z, y_hi = tm // 2, tm % 2
    depth = windows // 2
    x, y_lo, core = lat // 4, lat // 2 % 2, lat % 2
    y = 2 * y_hi + y_lo
    total = rows * bands
    tiles = rows // SUB
    pad = STEPS + 1
    span = rows + 2 * STEPS
    plane = rows * SUB

    def at(t, l):
        return {"tm": t, "lat": l}

    across = bands // 2
    slot = 2 * x + core

    def x_peer(d):
        i = lax.rem(slot + d, across)
        return at(tm, 4 * (i // 2) + 2 * y_lo + i % 2)

    mine = y * across + slot
    members = 4 * across

    def plane_peer(d):
        i = lax.rem(mine + d, members)
        j, k = i // across, i % across
        return at(2 * z + j // 2, 4 * (k // 2) + 2 * (j % 2) + k % 2)

    def y_peer(d):
        i = lax.rem(y + d, 4)
        return at(2 * z + i // 2, 4 * x + 2 * (i % 2) + core)

    def z_peer(d):
        return at(2 * lax.rem(z + d + depth, depth) + y_hi, lat)

    has_prev, has_next = tm > 0, tm < windows - 1
    has_south, has_north = lat > 0, lat < bands - 1
    prev_dev, next_dev = at(tm - 1, lat), at(tm + 1, lat)
    south_dev, north_dev = at(tm, lat - 1), at(tm, lat + 1)

    loads = [
        pltpu.make_async_copy(x_hbm, xin, local.at[0]),
        pltpu.make_async_copy(obs_hbm, obs, local.at[1]),
        pltpu.make_async_copy(cnt_hbm, cnt, local.at[2]),
    ]
    load_bg = pltpu.make_async_copy(bg_hbm, bg, local.at[3])
    loads[0].start()
    barrier = pltpu.get_barrier_semaphore()

    def greet(dev):
        pl.semaphore_signal(barrier, inc=1, device_id=dev, device_id_type=MESH)

    z_below, z_above = z > 0, z < depth - 1
    pl.when(z_below & (y_hi == 0))(lambda: greet(prev_dev))
    pl.when(z_above & (y_hi == 1))(lambda: greet(next_dev))
    pl.when(z_below)(lambda: greet(z_peer(-1)))
    pl.when(z_above)(lambda: greet(z_peer(1)))
    greet(at(tm, lax.rem(lat + 1, bands)))
    greet(at(tm, lax.rem(lat + bands - 1, bands)))
    for d in range(1, 4):
        greet(y_peer(d))
    for d in range(1, across):
        greet(x_peer(d))
    loads[1].start()
    loads[2].start()
    pl.when(tm == 0)(lambda: load_bg.start())

    row_tile = jnp.zeros((SUB, LANES), jnp.float32)

    def table(t, carry):
        index = lax.broadcasted_iota(jnp.int32, (SUB, LANES), 0) + (t * SUB + lat * rows - pad)
        f = spin_scale * jnp.sin(jnp.pi * ((index.astype(jnp.float32) + 0.5) / total - 0.5))
        for r in range(SUB):
            F[t * SUB + r] = jnp.broadcast_to(f[r : r + 1], (SUB, LANES))
        return carry

    lax.fori_loop(0, (span + 2 + SUB - 1) // SUB, table, 0)
    for c in range(3):
        for j in range(STEPS):
            S[j, c, 0] = row_tile
            S[j, c, span + 1] = row_tile
        for p in range(2):
            L[p, c, 0] = row_tile
            L[p, c, span + 1] = row_tile
        for b in range(1, pad):
            L[0, c, b] = row_tile
            L[0, c, b + rows + STEPS] = row_tile

    def zero_rows(ref, first):
        for c in range(3):
            for b in range(STEPS):
                ref[c, first + b] = row_tile

    def poles(ref):
        pl.when(lat == 0)(lambda: zero_rows(ref, 1))
        pl.when(lat == bands - 1)(lambda: zero_rows(ref, pad + rows))

    def tile_row(c, t, r):
        return pl.ds(c * plane + t * SUB * SUB + r, SUB, stride=SUB)

    def per_row(fn, carry=0):
        def body(t, carry):
            for r in range(SUB):
                carry = fn(t, r, carry)
            return carry

        return lax.fori_loop(0, tiles, body, carry)

    poles(S.at[0])
    loads[0].wait()

    def unpack(t, r, carry):
        for c in range(3):
            S[0, c, pad + t * SUB + r] = xin[tile_row(c, t, r), :]
        return carry

    per_row(unpack)
    before = (z + depth - 1) // depth
    after = (2 * depth - 2 - z) // depth
    facing = (1 - y_hi) * before + y_hi * after
    pl.semaphore_wait(barrier, 2 + 3 + across - 1 + before + after + facing)

    def remote(src, dst, k, dev):
        return pltpu.make_async_remote_copy(
            src_ref=src,
            dst_ref=dst,
            send_sem=send.at[k],
            recv_sem=recv.at[k],
            device_id=dev,
            device_id_type=MESH,
        )

    top = pl.ds(pad + rows - STEPS, STEPS)
    low = pl.ds(pad, STEPS)
    above = pl.ds(pad + rows, STEPS)
    below = pl.ds(1, STEPS)
    halo_up = remote(S.at[0, :, top], S.at[0, :, below], 0, north_dev)
    halo_down = remote(S.at[0, :, low], S.at[0, :, above], 1, south_dev)
    control = remote(xin, fol, 2, prev_dev)
    final = []
    for q in range(2):
        for c in range(3):
            k = len(final)
            final.append(
                pltpu.make_async_remote_copy(
                    src_ref=S.at[STEPS, c, pl.ds(pad + q * rows // 2, rows // 2)],
                    dst_ref=prev.at[c, pl.ds(q * rows // 2, rows // 2)],
                    send_sem=f_send.at[k],
                    recv_sem=f_recv.at[k],
                    device_id=next_dev,
                    device_id_type=MESH,
                )
            )
    out = 0
    edge_up = remote(L.at[out, :, above], edge.at[0], 3, north_dev)
    edge_down = remote(L.at[out, :, below], edge.at[1], 4, south_dev)

    pl.when(has_north)(lambda: halo_up.start())
    pl.when(has_south)(lambda: halo_down.start())
    pl.when(has_prev)(lambda: control.start())

    def z_signal(k):
        d = 2**k
        for exists, e in ((z >= d, -d), (z < depth - d, d)):

            @pl.when(exists)
            def _():
                pl.semaphore_signal(
                    z_sem.at[k], inc=1, device_id=z_peer(e), device_id_type=MESH
                )

    def z_wait(k):
        d = 2**k
        pl.semaphore_wait(z_sem.at[k], (z + depth - d) // depth + (2 * depth - 1 - d - z) // depth)

    z_signal(0)
    for d in range(1, across):
        pl.semaphore_signal(x_sem, inc=1, device_id=x_peer(d), device_id_type=MESH)
    pl.when(has_south)(lambda: halo_up.wait_recv())
    pl.when(has_north)(lambda: halo_down.wait_recv())

    def forward(j):
        def block(t, carry):
            b = 1 + t * BLOCK

            def rows_at(c, shift):
                return S[j, c, pl.ds(b + shift, BLOCK)]

            h, u, v = (rows_at(c, 0) for c in range(3))
            hn, un, vn = (rows_at(c, 1) for c in range(3))
            hs, us, vs = (rows_at(c, -1) for c in range(3))
            he, ue, ve = east(h), east(u), east(v)
            hw, uw, vw = west(h), west(u), west(v)
            f = F[pl.ds(b, BLOCK)]
            flux = ue * (1.0 + he) - uw * (1.0 + hw) + vn * (1.0 + hn) - vs * (1.0 + hs)
            S[j + 1, 0, pl.ds(b, BLOCK)] = (
                h - half * flux + diffusion * (hn + hs + he + hw - 4.0 * h)
            )
            S[j + 1, 1, pl.ds(b, BLOCK)] = (
                u
                - half * (he - hw + u * (ue - uw) + v * (un - us))
                + f * v
                + diffusion * (un + us + ue + uw - 4.0 * u)
            )
            S[j + 1, 2, pl.ds(b, BLOCK)] = (
                v
                - half * (hn - hs + u * (ve - vw) + v * (vn - vs))
                - f * u
                + diffusion * (vn + vs + ve + vw - 4.0 * v)
            )
            return carry

        lax.fori_loop(0, span // BLOCK, block, 0)
        poles(S.at[j + 1])

    for j in range(STEPS):
        forward(j)

    z_wait(0)
    z_signal(1)

    loads[1].wait()
    loads[2].wait()
    zero = jnp.zeros((SUB, LANES), jnp.float32)

    def observe(j):
        def fn(t, r, cost):
            resid = S[j + 1, 0, pad + t * SUB + r] - obs[tile_row(j, t, r), :]
            weighted = obs_weight * cnt[tile_row(j, t, r), :].astype(jnp.float32) * resid
            WR[j, t * SUB + r] = weighted
            return cost + weighted * resid

        return fn

    cost = zero
    for j in range(STEPS):
        cost = per_row(observe(j), cost)

    pl.when(has_prev)(lambda: control.wait_send())

    @pl.when(has_next & (y_hi == 0))
    def _():
        for piece in final[:EARLY]:
            piece.start()

    @pl.when(has_next)
    def _():
        control.wait_recv()

        def start(t, r, carry):
            i = t * SUB + r
            for c in range(3):
                back = S[STEPS, c, pad + i] - fol[tile_row(c, t, r), :]
                if c == 0:
                    back = back + WR[STEPS - 1, i]
                L[0, c, pad + i] = back
            return carry

        per_row(start)

    @pl.when(has_next & (y_hi == 1))
    def _():
        for piece in final[:EARLY]:
            piece.start()

    @pl.when(jnp.logical_not(has_next))
    def _():
        def start(t, r, carry):
            i = t * SUB + r
            L[0, 0, pad + i] = WR[STEPS - 1, i]
            L[0, 1, pad + i] = row_tile
            L[0, 2, pad + i] = row_tile
            return carry

        per_row(start)

    def backward(j, p):
        def block(t, carry):
            b = 1 + t * BLOCK

            def grads(c, shift):
                return L[p, c, pl.ds(b + shift, BLOCK)]

            def state(c, shift):
                return S[j, c, pl.ds(b + shift, BLOCK)]

            H, U, V = (grads(c, 0) for c in range(3))
            HN, UN, VN = (grads(c, 1) for c in range(3))
            HS, US, VS = (grads(c, -1) for c in range(3))
            HE, UE, VE = east(H), east(U), east(V)
            HW, UW, VW = west(H), west(U), west(V)
            h, u, v = (state(c, 0) for c in range(3))
            un, vn = state(1, 1), state(2, 1)
            us, vs = state(1, -1), state(2, -1)
            ue, ve = east(u), east(v)
            uw, vw = west(u), west(v)
            f = F[pl.ds(b, BLOCK)]
            along, across = HE - HW, HN - HS
            thick = 1.0 + h
            L[1 - p, 0, pl.ds(b, BLOCK)] = (
                H
                + half * (along * u + across * v + (UE - UW) + (VN - VS))
                + diffusion * (HN + HS + HE + HW - 4.0 * H)
            )
            L[1 - p, 1, pl.ds(b, BLOCK)] = (
                U
                - f * V
                + half
                * (
                    along * thick
                    - U * (ue - uw)
                    - V * (ve - vw)
                    + (UE * ue - UW * uw)
                    + (UN * vn - US * vs)
                )
                + diffusion * (UN + US + UE + UW - 4.0 * U)
            )
            L[1 - p, 2, pl.ds(b, BLOCK)] = (
                V
                + f * U
                + half
                * (
                    across * thick
                    - U * (un - us)
                    - V * (vn - vs)
                    + (VE * ue - VW * uw)
                    + (VN * vn - VS * vs)
                )
                + diffusion * (VN + VS + VE + VW - 4.0 * V)
            )
            return carry

        lax.fori_loop(0, span // BLOCK, block, 0)
        if j > 0:

            def inject(t, r, carry):
                i = t * SUB + r
                L[1 - p, 0, pad + i] = L[1 - p, 0, pad + i] + WR[j - 1, i]
                return carry

            per_row(inject)
            poles(L.at[1 - p])

    p = 0
    for j in reversed(range(STEPS)):
        backward(j, p)
        p = 1 - p

    pl.when(has_north)(lambda: edge_up.start())
    pl.when(has_south)(lambda: edge_down.start())

    @pl.when(has_next)
    def _():
        for piece in final[EARLY:]:
            piece.start()

    z_wait(1)
    z_signal(2)

    @pl.when(tm == 0)
    def _():
        load_bg.wait()

        def fn(t, r, carry):
            for c in range(3):
                prev[c, t * SUB + r] = bg[tile_row(c, t, r), :]
            return carry

        per_row(fn)

    @pl.when(has_south)
    def _():
        edge_up.wait_recv()
        for c in range(3):
            L[p, c, low] = L[p, c, low] + edge[0, c]

    @pl.when(has_north)
    def _():
        edge_down.wait_recv()
        for c in range(3):
            L[p, c, top] = L[p, c, top] + edge[1, c]

    pieces = []
    for q in range(2):
        for c in range(3):
            k = len(pieces)
            part = pl.ds(q * rows // 2, rows // 2)
            pieces.append(
                pltpu.make_async_remote_copy(
                    src_ref=L.at[p, c, pl.ds(pad + q * rows // 2, rows // 2)],
                    dst_ref=adjn.at[c, part],
                    send_sem=a_send.at[k],
                    recv_sem=a_recv.at[k],
                    device_id=prev_dev,
                    device_id_type=MESH,
                )
            )

    def send_pieces(first, last):
        @pl.when(has_prev)
        def _():
            for piece in pieces[first:last]:
                piece.start()

    z_wait(2)
    z_signal(3)

    @pl.when(has_prev)
    def _():
        for piece in final:
            piece.wait_recv()

    def gradient(t, r, carry):
        squares, cost = carry
        i = t * SUB + r
        for c in range(3):
            misfit = S[0, c, pad + i] - prev[c, i]
            g = misfit + L[p, c, pad + i]
            grad[tile_row(c, t, r), :] = g
            squares = squares + g * g
            cost = cost + misfit * misfit
        return squares, cost

    squares, cost = per_row(gradient, (zero, cost))

    def fold(x):
        x = jnp.sum(x, axis=0, keepdims=True)
        return x + pltpu.roll(x, LANES // 2, 1)

    lane = lax.broadcasted_iota(jnp.int32, (1, LANES), 1)
    pl.semaphore_wait(x_sem, across - 1)
    n1[mine] = jnp.where(lane < LANES // 2, fold(squares), fold(cost))

    def share(ref, i, k, dev):
        return pltpu.make_async_remote_copy(
            src_ref=ref.at[i],
            dst_ref=ref.at[i],
            send_sem=n_sem.at[k, 0],
            recv_sem=n_sem.at[k, 1],
            device_id=dev,
            device_id_type=MESH,
        )

    def share1(d, carry):
        share(n1, mine, 0, plane_peer(d)).start()
        return carry

    lax.fori_loop(1, members, share1, 0)

    @pl.when(has_next)
    def _():
        for piece in final:
            piece.wait_send()

    send_pieces(0, PACE)

    def settle(ref, count, k):
        many = pltpu.make_async_remote_copy(
            src_ref=ref.at[pl.ds(0, count)],
            dst_ref=ref.at[pl.ds(0, count)],
            send_sem=n_sem.at[k, 0],
            recv_sem=n_sem.at[k, 1],
            device_id=z_peer(1),
            device_id_type=MESH,
        )
        return many

    settle(n1, members - 1, 0).wait_recv()
    n2[z] = jnp.sum(n1[...], axis=0)
    z_wait(3)

    def share2(d, carry):
        share(n2, z, 1, z_peer(d)).start()
        return carry

    lax.fori_loop(1, depth, share2, 0)
    send_pieces(PACE, 6)

    @pl.when(has_next)
    def _():
        for piece in pieces:
            piece.wait_recv()

        def fn(t, r, carry):
            i = t * SUB + r
            for c in range(3):
                control = fol[tile_row(c, t, r), :]
                start_ref[tile_row(c, t, r), :] = control
                slope[tile_row(c, t, r), :] = (control - S[STEPS, c, pad + i]) + adjn[c, i]
            return carry

        per_row(fn)

    @pl.when(jnp.logical_not(has_next))
    def _():
        def fn(t, r, carry):
            for c in range(3):
                start_ref[tile_row(c, t, r), :] = S[STEPS, c, pad + t * SUB + r]
                slope[tile_row(c, t, r), :] = row_tile
            return carry

        per_row(fn)

    settle(n2, depth - 1, 1).wait_recv()
    sums = jnp.sum(n2[...], axis=0)
    square_total = jnp.sum(jnp.where(lane < LANES // 2, sums, 0.0), axis=1, keepdims=True)
    cost_total = jnp.sum(jnp.where(lane < LANES // 2, 0.0, sums), axis=1, keepdims=True)
    cost_ref[...] = jnp.broadcast_to(0.5 * cost_total, (SUB, LANES))
    scale = step_scale / jnp.sqrt(square_total / entries + epsilon)
    scale_ref[...] = jnp.broadcast_to(scale, (SUB, LANES))
    pl.when(has_north)(lambda: halo_up.wait_send())
    pl.when(has_south)(lambda: halo_down.wait_send())
    pl.when(has_north)(lambda: edge_up.wait_send())
    pl.when(has_south)(lambda: edge_down.wait_send())

    @pl.when(has_prev)
    def _():
        for piece in pieces:
            piece.wait_send()

    settle(n1, members - 1, 0).wait_send()
    settle(n2, depth - 1, 1).wait_send()


def finish(start, slope, grad, scale, cost, slid_hbm, grad_hbm, cost_ref, slid, sem):
    store_grad = pltpu.make_async_copy(grad, grad_hbm, sem.at[CHUNKS])
    store_grad.start()
    rows = slid.shape[0] // CHUNKS
    s = jnp.broadcast_to(scale[0:1], (rows, LANES))
    stores = []
    for q in range(CHUNKS):
        part = pl.ds(q * rows, rows)
        slid[part] = start[part] - s * slope[part]
        stores.append(pltpu.make_async_copy(slid.at[part], slid_hbm.at[part], sem.at[q]))
        stores[-1].start()
    cost_ref[0, 0] = jnp.max(cost[...])
    for store in stores:
        store.wait()
    store_grad.wait()


def to_tiles(x):
    c, rows, lon = x.shape
    x = x.reshape(c, rows // SUB, SUB, lon // LANES, LANES)
    return x.transpose(0, 1, 3, 2, 4).reshape(c * rows * lon // LANES, LANES)


def from_tiles(x, rows, lon):
    x = x.reshape(-1, rows // SUB, lon // LANES, SUB, LANES)
    return x.transpose(0, 1, 3, 2, 4).reshape(-1, rows, lon)


def per_device(controls, background, observations, obs_count):
    rows, lon = controls.shape[2:]
    windows, bands = lax.axis_size("tm"), lax.axis_size("lat")
    entries = float(windows * bands * controls[0].size)
    n = 3 * rows * lon // LANES
    m = STEPS * rows * lon // LANES
    high = rows + 2 * STEPS + 2
    vmem = lambda *shape: pltpu.VMEM(shape, jnp.float32)
    dma = pltpu.SemaphoreType.DMA
    held = pltpu.VMEM((n, LANES), jnp.float32)
    tile = pltpu.VMEM((SUB, LANES), jnp.float32)
    stored = jax.ShapeDtypeStruct((n, LANES), jnp.float32)
    whole = pl.BlockSpec(memory_space=pltpu.VMEM)
    anywhere = pl.BlockSpec(memory_space=pl.ANY)
    results = pl.pallas_call(
        functools.partial(kernel, windows, bands, rows, entries),
        out_shape=(held, held, held, tile, tile),
        in_specs=[anywhere] * 4,
        out_specs=(whole,) * 5,
        scratch_shapes=[
            vmem(n, LANES),
            vmem(n, LANES),
            vmem(m, LANES),
            pltpu.VMEM((m, LANES), jnp.int32),
            vmem(n, LANES),
            vmem(STEPS + 1, 3, high, SUB, LANES),
            vmem(2, 3, high, SUB, LANES),
            vmem(STEPS, rows, SUB, LANES),
            vmem((high + SUB - 1) // SUB * SUB, SUB, LANES),
            vmem(3, rows, SUB, LANES),
            vmem(3, rows, SUB, LANES),
            vmem(2, 3, STEPS, SUB, LANES),
            vmem(2 * bands, 1, LANES),
            vmem(windows // 2, 1, LANES),
            dma((4,)),
            dma((5,)),
            dma((5,)),
            dma((6,)),
            dma((6,)),
            dma((6,)),
            dma((6,)),
            dma((2, 2)),
            pltpu.SemaphoreType.REGULAR((4,)),
            pltpu.SemaphoreType.REGULAR,
        ],
        compiler_params=pltpu.CompilerParams(collective_id=0, has_side_effects=True),
    )(
        to_tiles(controls[0]),
        to_tiles(background),
        to_tiles(observations[0]),
        to_tiles(obs_count[0]),
    )
    slid, grad, cost = pl.pallas_call(
        finish,
        out_shape=(stored, stored, jax.ShapeDtypeStruct((1, 1), jnp.float32)),
        in_specs=[whole] * 5,
        out_specs=(anywhere, anywhere, pl.BlockSpec(memory_space=pltpu.SMEM)),
        scratch_shapes=[vmem(n, LANES), dma((CHUNKS + 1,))],
    )(*(pltpu.with_memory_space_constraint(r, pltpu.VMEM) for r in results))
    return (
        from_tiles(slid, rows, lon)[None],
        from_tiles(grad, rows, lon)[None],
        cost[0, 0],
    )


def solution(mesh):
    spec = P("tm", None, "lat", None)
    return jax.shard_map(
        per_device,
        mesh=mesh,
        in_specs=(spec, P(None, "lat", None), spec, spec),
        out_specs=(spec, spec, P()),
        check_vma=False,
    )
```

```python
import functools

import jax
import jax.numpy as jnp
from jax import lax
from jax.experimental import pallas as pl
from jax.experimental.pallas import tpu as pltpu
from jax.sharding import PartitionSpec as P

half = 0.125
diffusion = 0.1
spin_scale = 0.3
obs_weight = 0.5
step_scale = 0.2
epsilon = 1e-06

STEPS = 4
SUB, LANES = 8, 128
BLOCK = 20
CHUNKS = 3
EARLY = 3
PACE = 4
MESH = pl.DeviceIdType.MESH


def east(x):
    near = pltpu.roll(x, LANES - 1, x.ndim - 1)
    far = pltpu.roll(near, SUB - 1, x.ndim - 2)
    lane = lax.broadcasted_iota(jnp.int32, x.shape, x.ndim - 1)
    return jnp.where(lane == LANES - 1, far, near)


def west(x):
    near = pltpu.roll(x, 1, x.ndim - 1)
    far = pltpu.roll(near, 1, x.ndim - 2)
    lane = lax.broadcasted_iota(jnp.int32, x.shape, x.ndim - 1)
    return jnp.where(lane == 0, far, near)


def kernel(
    windows,
    bands,
    rows,
    entries,
    x_hbm,
    bg_hbm,
    obs_hbm,
    cnt_hbm,
    start_ref,
    slope,
    grad,
    scale_ref,
    cost_ref,
    xin,
    bg,
    obs,
    cnt,
    fol,
    S,
    L,
    WR,
    F,
    prev,
    adjn,
    edge,
    n1,
    n2,
    local,
    send,
    recv,
    f_send,
    f_recv,
    a_send,
    a_recv,
    n_sem,
    z_sem,
    x_sem,
):
    tm, lat = lax.axis_index("tm"), lax.axis_index("lat")
    z, y_hi = tm // 2, tm % 2
    depth = windows // 2
    x, y_lo, core = lat // 4, lat // 2 % 2, lat % 2
    y = 2 * y_hi + y_lo
    total = rows * bands
    tiles = rows // SUB
    pad = STEPS + 1
    span = rows + 2 * STEPS
    plane = rows * SUB

    def at(t, l):
        return {"tm": t, "lat": l}

    across = bands // 2
    slot = 2 * x + core

    def x_peer(d):
        i = lax.rem(slot + d, across)
        return at(tm, 4 * (i // 2) + 2 * y_lo + i % 2)

    mine = y * across + slot
    members = 4 * across

    def plane_peer(d):
        i = lax.rem(mine + d, members)
        j, k = lax.div(i, across), lax.rem(i, across)
        x_core = lax.rem(k, 2) + 4 * lax.div(k, 2)
        return at(2 * z + lax.div(j, 2), x_core + 2 * lax.rem(j, 2))

    def y_peer(d):
        i = lax.rem(y + d, 4)
        return at(2 * z + i // 2, 4 * x + 2 * (i % 2) + core)

    def z_peer(d):
        return at(2 * lax.rem(z + d + depth, depth) + y_hi, lat)

    has_prev, has_next = tm > 0, tm < windows - 1
    has_south, has_north = lat > 0, lat < bands - 1
    prev_dev, next_dev = at(tm - 1, lat), at(tm + 1, lat)
    south_dev, north_dev = at(tm, lat - 1), at(tm, lat + 1)

    loads = [
        pltpu.make_async_copy(x_hbm, xin, local.at[0]),
        pltpu.make_async_copy(obs_hbm, obs, local.at[1]),
        pltpu.make_async_copy(cnt_hbm, cnt, local.at[2]),
    ]
    load_bg = pltpu.make_async_copy(bg_hbm, bg, local.at[3])
    loads[0].start()
    barrier = pltpu.get_barrier_semaphore()

    def greet(dev):
        pl.semaphore_signal(barrier, inc=1, device_id=dev, device_id_type=MESH)

    z_below, z_above = z > 0, z < depth - 1
    pl.when(z_below & (y_hi == 0))(lambda: greet(prev_dev))
    pl.when(z_above & (y_hi == 1))(lambda: greet(next_dev))
    pl.when(z_below)(lambda: greet(z_peer(-1)))
    pl.when(z_above)(lambda: greet(z_peer(1)))
    greet(at(tm, lax.rem(lat + 1, bands)))
    greet(at(tm, lax.rem(lat + bands - 1, bands)))
    for d in range(1, 4):
        greet(y_peer(d))
    for d in range(1, across):
        greet(x_peer(d))
    loads[1].start()
    loads[2].start()
    pl.when(tm == 0)(lambda: load_bg.start())

    row_tile = jnp.zeros((SUB, LANES), jnp.float32)

    def table(t, carry):
        index = lax.broadcasted_iota(jnp.int32, (SUB, LANES), 0) + (t * SUB + lat * rows - pad)
        f = spin_scale * jnp.sin(jnp.pi * ((index.astype(jnp.float32) + 0.5) / total - 0.5))
        for r in range(SUB):
            F[t * SUB + r] = jnp.broadcast_to(f[r : r + 1], (SUB, LANES))
        return carry

    lax.fori_loop(0, (span + 2 + SUB - 1) // SUB, table, 0)
    for c in range(3):
        for j in range(STEPS):
            S[j, c, 0] = row_tile
            S[j, c, span + 1] = row_tile
        for p in range(2):
            L[p, c, 0] = row_tile
            L[p, c, span + 1] = row_tile
        for b in range(1, pad):
            L[0, c, b] = row_tile
            L[0, c, b + rows + STEPS] = row_tile

    def zero_rows(ref, first):
        for c in range(3):
            for b in range(STEPS):
                ref[c, first + b] = row_tile

    def poles(ref):
        pl.when(lat == 0)(lambda: zero_rows(ref, 1))
        pl.when(lat == bands - 1)(lambda: zero_rows(ref, pad + rows))

    def tile_row(c, t, r):
        return pl.ds(c * plane + t * SUB * SUB + r, SUB, stride=SUB)

    def per_row(fn, carry=0):
        def body(t, carry):
            for r in range(SUB):
                carry = fn(t, r, carry)
            return carry

        return lax.fori_loop(0, tiles, body, carry)

    poles(S.at[0])
    loads[0].wait()

    def unpack(t, r, carry):
        for c in range(3):
            S[0, c, pad + t * SUB + r] = xin[tile_row(c, t, r), :]
        return carry

    per_row(unpack)
    before = (z + depth - 1) // depth
    after = (2 * depth - 2 - z) // depth
    facing = (1 - y_hi) * before + y_hi * after
    pl.semaphore_wait(barrier, 2 + 3 + across - 1 + before + after + facing)

    def remote(src, dst, k, dev):
        return pltpu.make_async_remote_copy(
            src_ref=src,
            dst_ref=dst,
            send_sem=send.at[k],
            recv_sem=recv.at[k],
            device_id=dev,
            device_id_type=MESH,
        )

    top = pl.ds(pad + rows - STEPS, STEPS)
    low = pl.ds(pad, STEPS)
    above = pl.ds(pad + rows, STEPS)
    below = pl.ds(1, STEPS)
    halo_up = remote(S.at[0, :, top], S.at[0, :, below], 0, north_dev)
    halo_down = remote(S.at[0, :, low], S.at[0, :, above], 1, south_dev)
    control = remote(xin, fol, 2, prev_dev)
    final = []
    for q in range(2):
        for c in range(3):
            k = len(final)
            final.append(
                pltpu.make_async_remote_copy(
                    src_ref=S.at[STEPS, c, pl.ds(pad + q * rows // 2, rows // 2)],
                    dst_ref=prev.at[c, pl.ds(q * rows // 2, rows // 2)],
                    send_sem=f_send.at[k],
                    recv_sem=f_recv.at[k],
                    device_id=next_dev,
                    device_id_type=MESH,
                )
            )
    out = 0
    edge_up = remote(L.at[out, :, above], edge.at[0], 3, north_dev)
    edge_down = remote(L.at[out, :, below], edge.at[1], 4, south_dev)

    pl.when(has_north)(lambda: halo_up.start())
    pl.when(has_south)(lambda: halo_down.start())
    pl.when(has_prev)(lambda: control.start())

    def z_signal(k):
        d = 2**k
        for exists, e in ((z >= d, -d), (z < depth - d, d)):

            @pl.when(exists)
            def _():
                pl.semaphore_signal(
                    z_sem.at[k], inc=1, device_id=z_peer(e), device_id_type=MESH
                )

    def z_wait(k):
        d = 2**k
        pl.semaphore_wait(z_sem.at[k], (z + depth - d) // depth + (2 * depth - 1 - d - z) // depth)

    z_signal(0)
    for d in range(1, across):
        pl.semaphore_signal(x_sem, inc=1, device_id=x_peer(d), device_id_type=MESH)
    pl.when(has_south)(lambda: halo_up.wait_recv())
    pl.when(has_north)(lambda: halo_down.wait_recv())

    def forward(j):
        def block(t, carry):
            b = 1 + t * BLOCK

            def rows_at(c, shift):
                return S[j, c, pl.ds(b + shift, BLOCK)]

            h, u, v = (rows_at(c, 0) for c in range(3))
            hn, un, vn = (rows_at(c, 1) for c in range(3))
            hs, us, vs = (rows_at(c, -1) for c in range(3))
            he, ue, ve = east(h), east(u), east(v)
            hw, uw, vw = west(h), west(u), west(v)
            f = F[pl.ds(b, BLOCK)]
            flux = ue * (1.0 + he) - uw * (1.0 + hw) + vn * (1.0 + hn) - vs * (1.0 + hs)
            S[j + 1, 0, pl.ds(b, BLOCK)] = (
                h - half * flux + diffusion * (hn + hs + he + hw - 4.0 * h)
            )
            S[j + 1, 1, pl.ds(b, BLOCK)] = (
                u
                - half * (he - hw + u * (ue - uw) + v * (un - us))
                + f * v
                + diffusion * (un + us + ue + uw - 4.0 * u)
            )
            S[j + 1, 2, pl.ds(b, BLOCK)] = (
                v
                - half * (hn - hs + u * (ve - vw) + v * (vn - vs))
                - f * u
                + diffusion * (vn + vs + ve + vw - 4.0 * v)
            )
            return carry

        lax.fori_loop(0, span // BLOCK, block, 0)
        poles(S.at[j + 1])

    for j in range(STEPS):
        forward(j)

    z_wait(0)
    z_signal(1)

    loads[1].wait()
    loads[2].wait()
    zero = jnp.zeros((SUB, LANES), jnp.float32)

    def observe(j):
        def fn(t, r, cost):
            resid = S[j + 1, 0, pad + t * SUB + r] - obs[tile_row(j, t, r), :]
            weighted = obs_weight * cnt[tile_row(j, t, r), :].astype(jnp.float32) * resid
            WR[j, t * SUB + r] = weighted
            return cost + weighted * resid

        return fn

    cost = zero
    for j in range(STEPS):
        cost = per_row(observe(j), cost)

    pl.when(has_prev)(lambda: control.wait_send())

    @pl.when(has_next & (y_hi == 0))
    def _():
        for piece in final:
            piece.start()

    @pl.when(has_next)
    def _():
        control.wait_recv()

        def start(t, r, carry):
            i = t * SUB + r
            for c in range(3):
                back = S[STEPS, c, pad + i] - fol[tile_row(c, t, r), :]
                if c == 0:
                    back = back + WR[STEPS - 1, i]
                L[0, c, pad + i] = back
            return carry

        per_row(start)

    @pl.when(has_next & (y_hi == 1))
    def _():
        for piece in final[:EARLY]:
            piece.start()

    @pl.when(jnp.logical_not(has_next))
    def _():
        def start(t, r, carry):
            i = t * SUB + r
            L[0, 0, pad + i] = WR[STEPS - 1, i]
            L[0, 1, pad + i] = row_tile
            L[0, 2, pad + i] = row_tile
            return carry

        per_row(start)

    def backward(j, p):
        def block(t, carry):
            b = 1 + t * BLOCK

            def grads(c, shift):
                return L[p, c, pl.ds(b + shift, BLOCK)]

            def state(c, shift):
                return S[j, c, pl.ds(b + shift, BLOCK)]

            H, U, V = (grads(c, 0) for c in range(3))
            HN, UN, VN = (grads(c, 1) for c in range(3))
            HS, US, VS = (grads(c, -1) for c in range(3))
            HE, UE, VE = east(H), east(U), east(V)
            HW, UW, VW = west(H), west(U), west(V)
            h, u, v = (state(c, 0) for c in range(3))
            un, vn = state(1, 1), state(2, 1)
            us, vs = state(1, -1), state(2, -1)
            ue, ve = east(u), east(v)
            uw, vw = west(u), west(v)
            f = F[pl.ds(b, BLOCK)]
            along, across = HE - HW, HN - HS
            thick = 1.0 + h
            L[1 - p, 0, pl.ds(b, BLOCK)] = (
                H
                + half * (along * u + across * v + (UE - UW) + (VN - VS))
                + diffusion * (HN + HS + HE + HW - 4.0 * H)
            )
            L[1 - p, 1, pl.ds(b, BLOCK)] = (
                U
                - f * V
                + half
                * (
                    along * thick
                    - U * (ue - uw)
                    - V * (ve - vw)
                    + (UE * ue - UW * uw)
                    + (UN * vn - US * vs)
                )
                + diffusion * (UN + US + UE + UW - 4.0 * U)
            )
            L[1 - p, 2, pl.ds(b, BLOCK)] = (
                V
                + f * U
                + half
                * (
                    across * thick
                    - U * (un - us)
                    - V * (vn - vs)
                    + (VE * ue - VW * uw)
                    + (VN * vn - VS * vs)
                )
                + diffusion * (VN + VS + VE + VW - 4.0 * V)
            )
            return carry

        lax.fori_loop(0, span // BLOCK, block, 0)
        if j > 0:

            def inject(t, r, carry):
                i = t * SUB + r
                L[1 - p, 0, pad + i] = L[1 - p, 0, pad + i] + WR[j - 1, i]
                return carry

            per_row(inject)
            poles(L.at[1 - p])

    p = 0
    for j in reversed(range(STEPS)):
        backward(j, p)
        p = 1 - p

    pl.when(has_north)(lambda: edge_up.start())
    pl.when(has_south)(lambda: edge_down.start())

    @pl.when(has_next & (y_hi == 1))
    def _():
        for piece in final[EARLY:]:
            piece.start()

    z_wait(1)
    z_signal(2)

    @pl.when(tm == 0)
    def _():
        load_bg.wait()

        def fn(t, r, carry):
            for c in range(3):
                prev[c, t * SUB + r] = bg[tile_row(c, t, r), :]
            return carry

        per_row(fn)

    @pl.when(has_south)
    def _():
        edge_up.wait_recv()
        for c in range(3):
            L[p, c, low] = L[p, c, low] + edge[0, c]

    @pl.when(has_north)
    def _():
        edge_down.wait_recv()
        for c in range(3):
            L[p, c, top] = L[p, c, top] + edge[1, c]

    pieces = []
    for q in range(2):
        for c in range(3):
            k = len(pieces)
            part = pl.ds(q * rows // 2, rows // 2)
            pieces.append(
                pltpu.make_async_remote_copy(
                    src_ref=L.at[p, c, pl.ds(pad + q * rows // 2, rows // 2)],
                    dst_ref=adjn.at[c, part],
                    send_sem=a_send.at[k],
                    recv_sem=a_recv.at[k],
                    device_id=prev_dev,
                    device_id_type=MESH,
                )
            )

    def send_pieces(first, last):
        @pl.when(has_prev)
        def _():
            for piece in pieces[first:last]:
                piece.start()

    z_wait(2)
    z_signal(3)

    @pl.when(has_prev)
    def _():
        for piece in final:
            piece.wait_recv()

    def gradient(t, r, carry):
        squares, cost = carry
        i = t * SUB + r
        for c in range(3):
            misfit = S[0, c, pad + i] - prev[c, i]
            g = misfit + L[p, c, pad + i]
            grad[tile_row(c, t, r), :] = g
            squares = squares + g * g
            cost = cost + misfit * misfit
        return squares, cost

    squares, cost = per_row(gradient, (zero, cost))

    def fold(x):
        x = jnp.sum(x, axis=0, keepdims=True)
        return x + pltpu.roll(x, LANES // 2, 1)

    lane = lax.broadcasted_iota(jnp.int32, (1, LANES), 1)
    pl.semaphore_wait(x_sem, across - 1)
    n1[mine] = jnp.where(lane < LANES // 2, fold(squares), fold(cost))

    def share(ref, i, k, dev):
        return pltpu.make_async_remote_copy(
            src_ref=ref.at[i],
            dst_ref=ref.at[i],
            send_sem=n_sem.at[k, 0],
            recv_sem=n_sem.at[k, 1],
            device_id=dev,
            device_id_type=MESH,
        )

    def share1(d, carry):
        share(n1, mine, 0, plane_peer(d)).start()
        return carry

    lax.fori_loop(1, members, share1, 0)

    @pl.when(has_next)
    def _():
        for piece in final:
            piece.wait_send()

    send_pieces(0, PACE)

    def settle(ref, count, k):
        many = pltpu.make_async_remote_copy(
            src_ref=ref.at[pl.ds(0, count)],
            dst_ref=ref.at[pl.ds(0, count)],
            send_sem=n_sem.at[k, 0],
            recv_sem=n_sem.at[k, 1],
            device_id=z_peer(1),
            device_id_type=MESH,
        )
        return many

    settle(n1, members - 1, 0).wait_recv()
    n2[z] = jnp.sum(n1[...], axis=0)
    z_wait(3)

    def share2(d, carry):
        share(n2, z, 1, z_peer(d)).start()
        return carry

    lax.fori_loop(1, depth, share2, 0)
    send_pieces(PACE, 6)

    @pl.when(has_next)
    def _():
        for piece in pieces:
            piece.wait_recv()

        def fn(t, r, carry):
            i = t * SUB + r
            for c in range(3):
                control = fol[tile_row(c, t, r), :]
                start_ref[tile_row(c, t, r), :] = control
                slope[tile_row(c, t, r), :] = (control - S[STEPS, c, pad + i]) + adjn[c, i]
            return carry

        per_row(fn)

    @pl.when(jnp.logical_not(has_next))
    def _():
        def fn(t, r, carry):
            for c in range(3):
                start_ref[tile_row(c, t, r), :] = S[STEPS, c, pad + t * SUB + r]
                slope[tile_row(c, t, r), :] = row_tile
            return carry

        per_row(fn)

    settle(n2, depth - 1, 1).wait_recv()
    sums = jnp.sum(n2[...], axis=0)
    square_total = jnp.sum(jnp.where(lane < LANES // 2, sums, 0.0), axis=1, keepdims=True)
    cost_total = jnp.sum(jnp.where(lane < LANES // 2, 0.0, sums), axis=1, keepdims=True)
    cost_ref[...] = jnp.broadcast_to(0.5 * cost_total, (SUB, LANES))
    scale = step_scale / jnp.sqrt(square_total / entries + epsilon)
    scale_ref[...] = jnp.broadcast_to(scale, (SUB, LANES))
    pl.when(has_north)(lambda: halo_up.wait_send())
    pl.when(has_south)(lambda: halo_down.wait_send())
    pl.when(has_north)(lambda: edge_up.wait_send())
    pl.when(has_south)(lambda: edge_down.wait_send())

    @pl.when(has_prev)
    def _():
        for piece in pieces:
            piece.wait_send()

    settle(n1, members - 1, 0).wait_send()
    settle(n2, depth - 1, 1).wait_send()


def finish(start, slope, grad, scale, cost, slid_hbm, grad_hbm, cost_ref, slid, sem):
    store_grad = pltpu.make_async_copy(grad, grad_hbm, sem.at[CHUNKS])
    store_grad.start()
    rows = slid.shape[0] // CHUNKS
    s = jnp.broadcast_to(scale[0:1], (rows, LANES))
    stores = []
    for q in range(CHUNKS):
        part = pl.ds(q * rows, rows)
        slid[part] = start[part] - s * slope[part]
        stores.append(pltpu.make_async_copy(slid.at[part], slid_hbm.at[part], sem.at[q]))
        stores[-1].start()
    cost_ref[0, 0] = jnp.max(cost[...])
    for store in stores:
        store.wait()
    store_grad.wait()


def to_tiles(x):
    c, rows, lon = x.shape
    x = x.reshape(c, rows // SUB, SUB, lon // LANES, LANES)
    return x.transpose(0, 1, 3, 2, 4).reshape(c * rows * lon // LANES, LANES)


def from_tiles(x, rows, lon):
    x = x.reshape(-1, rows // SUB, lon // LANES, SUB, LANES)
    return x.transpose(0, 1, 3, 2, 4).reshape(-1, rows, lon)


def per_device(controls, background, observations, obs_count):
    rows, lon = controls.shape[2:]
    windows, bands = lax.axis_size("tm"), lax.axis_size("lat")
    entries = float(windows * bands * controls[0].size)
    n = 3 * rows * lon // LANES
    m = STEPS * rows * lon // LANES
    high = rows + 2 * STEPS + 2
    vmem = lambda *shape: pltpu.VMEM(shape, jnp.float32)
    dma = pltpu.SemaphoreType.DMA
    held = pltpu.VMEM((n, LANES), jnp.float32)
    tile = pltpu.VMEM((SUB, LANES), jnp.float32)
    stored = jax.ShapeDtypeStruct((n, LANES), jnp.float32)
    whole = pl.BlockSpec(memory_space=pltpu.VMEM)
    anywhere = pl.BlockSpec(memory_space=pl.ANY)
    results = pl.pallas_call(
        functools.partial(kernel, windows, bands, rows, entries),
        out_shape=(held, held, held, tile, tile),
        in_specs=[anywhere] * 4,
        out_specs=(whole,) * 5,
        scratch_shapes=[
            vmem(n, LANES),
            vmem(n, LANES),
            vmem(m, LANES),
            pltpu.VMEM((m, LANES), jnp.int32),
            vmem(n, LANES),
            vmem(STEPS + 1, 3, high, SUB, LANES),
            vmem(2, 3, high, SUB, LANES),
            vmem(STEPS, rows, SUB, LANES),
            vmem((high + SUB - 1) // SUB * SUB, SUB, LANES),
            vmem(3, rows, SUB, LANES),
            vmem(3, rows, SUB, LANES),
            vmem(2, 3, STEPS, SUB, LANES),
            vmem(2 * bands, 1, LANES),
            vmem(windows // 2, 1, LANES),
            dma((4,)),
            dma((5,)),
            dma((5,)),
            dma((6,)),
            dma((6,)),
            dma((6,)),
            dma((6,)),
            dma((2, 2)),
            pltpu.SemaphoreType.REGULAR((4,)),
            pltpu.SemaphoreType.REGULAR,
        ],
        compiler_params=pltpu.CompilerParams(collective_id=0, has_side_effects=True),
    )(
        to_tiles(controls[0]),
        to_tiles(background),
        to_tiles(observations[0]),
        to_tiles(obs_count[0]),
    )
    slid, grad, cost = pl.pallas_call(
        finish,
        out_shape=(stored, stored, jax.ShapeDtypeStruct((1, 1), jnp.float32)),
        in_specs=[whole] * 5,
        out_specs=(anywhere, anywhere, pl.BlockSpec(memory_space=pltpu.SMEM)),
        scratch_shapes=[vmem(n, LANES), dma((CHUNKS + 1,))],
    )(*(pltpu.with_memory_space_constraint(r, pltpu.VMEM) for r in results))
    return (
        from_tiles(slid, rows, lon)[None],
        from_tiles(grad, rows, lon)[None],
        cost[0, 0],
    )


def solution(mesh):
    spec = P("tm", None, "lat", None)
    return jax.shard_map(
        per_device,
        mesh=mesh,
        in_specs=(spec, P(None, "lat", None), spec, spec),
        out_specs=(spec, spec, P()),
        check_vma=False,
    )
```
